16 devices in a mesh: dp: 2 (over y, z), tp: 8 (over x, core).
Axes of the slice: x: 4, y: 2, z: 1, core: 2. Of those that a mesh axis runs over, the one named last changes fastest.
The devices are a block of a 4x4x8 slice.
Arguments:
- x: bfloat16 [4096, 7168], P(('dp', 'tp')), parts along dimension 0
- dy: bfloat16 [4096, 7168], P(('dp', 'tp')), parts along dimension 0
- gain: bfloat16 [7168], replicated
- wq: bfloat16 [7168, 7168], P(None, 'tp')
- wk: bfloat16 [7168, 1024], P(None, 'tp')
- wv: bfloat16 [7168, 1024], P(None, 'tp')
- wo: bfloat16 [7168, 7168], P('tp')
Outputs:
- output 1: bfloat16 [4096, 7168], P(('dp', 'tp')), parts along dimension 0
- output 2: float32 [2, 7168], P('dp'), parts along dimension 0
- output 3: bfloat16 [14336, 7168], P('dp', 'tp'), parts along dimension 0
- output 4: bfloat16 [14336, 1024], P('dp', 'tp'), parts along dimension 0
- output 5: bfloat16 [14336, 1024], P('dp', 'tp'), parts along dimension 0
- output 6: bfloat16 [14336, 7168], P(('dp', 'tp')), parts along dimension 0
There are 2 independent parts. The reference program is written for one: setup_inputs(seed, part) draws one part's arguments, and reference() takes and returns one part's arrays. A program takes and returns all parts, laid end to end along the dimension named above; an argument that names none is the same for every part.
All inputs are finite; a program needn't handle non-finite values.
Results may differ from the reference program's by a relative error of at most 0.018.
Values are sent between devices in bfloat16 or wider.
A program may use at most 768 MiB of HBM per device.

```python
import jax
import jax.numpy as jnp
from jax import lax

ROWS = 2048
D = 7168
HEADS = 56
KV_HEADS = 8
HEAD = 128
THETA = 10000


def setup_inputs(seed: int = 0, part: int = 0) -> dict:
    kx, ky, kn, kq, kk, kv, ko = jax.random.split(jax.random.key(seed), 7)

    def weights(key, rows, columns):
        return jax.random.normal(key, (rows, columns), jnp.float32) * rows**-0.5

    drawn = {
        "x": jax.random.normal(jax.random.fold_in(kx, part), (ROWS, D), jnp.float32),
        "dy": jax.random.normal(jax.random.fold_in(ky, part), (ROWS, D), jnp.float32) * ROWS**-0.5,
        "gain": 1 + 0.1 * jax.random.normal(kn, (D,), jnp.float32),
        "wq": 2 * weights(kq, D, HEADS * HEAD),
        "wk": 2 * weights(kk, D, KV_HEADS * HEAD),
        "wv": 4 * weights(kv, D, KV_HEADS * HEAD),
        "wo": weights(ko, HEADS * HEAD, D),
    }
    return {k: v.astype(jnp.bfloat16) for k, v in drawn.items()}


def normed(x, gain):
    wide = x.astype(jnp.float32)
    scale = lax.rsqrt(jnp.mean(wide * wide, -1, keepdims=True) + 1e-6)
    return (wide * scale * gain.astype(jnp.float32)).astype(jnp.bfloat16)


def turned(t, place, theta):
    half = t.shape[-1] // 2
    angle = place.astype(jnp.float32)[:, None] * theta ** (-jnp.arange(half, dtype=jnp.float32) / half)
    cos, sin = jnp.cos(angle)[:, None], jnp.sin(angle)[:, None]
    a, b = t[..., :half].astype(jnp.float32), t[..., half:].astype(jnp.float32)
    return jnp.concatenate([a * cos - b * sin, b * cos + a * sin], -1).astype(jnp.bfloat16)


def matmul(a, w):
    return jnp.dot(a, w, preferred_element_type=jnp.float32).astype(jnp.bfloat16)


def einsum(form, a, b):
    return jnp.einsum(form, a.astype(jnp.float32), b.astype(jnp.float32))


def attention(q, k, v):
    scores = einsum("tgsd,ugd->gstu", q, k) * q.shape[-1] ** -0.5
    token = jnp.arange(q.shape[0])
    scores = jnp.where(token[:, None] >= token, scores, -jnp.inf)
    weights = jax.nn.softmax(scores, -1).astype(jnp.bfloat16)
    return einsum("gstu,ugd->tgsd", weights, v).astype(jnp.bfloat16)


def forward(x, gain, wq, wk, wv, wo):
    rows = x.shape[0]
    a, place = normed(x, gain), jnp.arange(rows)
    k = turned(matmul(a, wk).reshape(rows, -1, HEAD), place, THETA)
    q = turned(matmul(a, wq).reshape(rows, -1, HEAD), place, THETA).reshape(rows, k.shape[1], -1, HEAD)
    v = matmul(a, wv).reshape(rows, -1, HEAD)
    seen = attention(q, k, v).reshape(rows, -1)
    return (x.astype(jnp.float32) + jnp.dot(seen, wo, preferred_element_type=jnp.float32)).astype(jnp.bfloat16)


def reference(x, dy, gain, wq, wk, wv, wo):
    _, back = jax.vjp(forward, x, gain.astype(jnp.float32), wq, wk, wv, wo)
    by_x, by_gain, *by_weights = back(dy)
    return (by_x, by_gain[None], *by_weights)
```

```python
import functools

import jax
import jax.numpy as jnp
from jax import lax
from jax.experimental import pallas as pl
from jax.experimental.pallas import tpu as pltpu
from jax.sharding import PartitionSpec as P

NEG = -1e30
HIDDEN = 2 * NEG
LOG2E = 1.4426950408889634
VMEM = 62 * 2**20
HEAD = 128
THETA = 10000
PARTS = 2
DEVS = 2
BK = 512
COLS = 4


def _dot(a, b, ca, cb):
    return lax.dot_general(a, b, (((ca,), (cb,)), ((), ())), preferred_element_type=jnp.float32)


def _whole(shape):
    return pl.BlockSpec(shape, lambda *_: (0,) * len(shape), pipeline_mode=pl.Buffered(1))


def _params(n=1):
    return pltpu.CompilerParams(dimension_semantics=("arbitrary",) * n, vmem_limit_bytes=VMEM)


def _cost(flops, arrays, exps=0):
    return pl.CostEstimate(flops=int(flops), transcendentals=int(exps), bytes_accessed=sum(a.size * a.dtype.itemsize for a in arrays))


def _like(shape, dtype=jnp.bfloat16):
    return jax.ShapeDtypeStruct(shape, dtype)


def normed(x, gain):
    wide = x.astype(jnp.float32)
    scale = lax.rsqrt(jnp.mean(wide * wide, -1, keepdims=True) + 1e-6)
    return (wide * scale * gain.astype(jnp.float32)).astype(jnp.bfloat16)


def _turn(t, cos, sin):
    t = t.astype(jnp.bfloat16).astype(jnp.float32)
    return (t * cos + pltpu.roll(t, HEAD // 2, 1) * sin).astype(jnp.bfloat16)


def _qkv_kernel(a_ref, wq_ref, wk_ref, wv_ref, cos_ref, sin_ref, q_ref, k_ref, v_ref):
    a = a_ref[...]
    cos, sin = cos_ref[...], sin_ref[...]
    q = _dot(a, wq_ref[...], 1, 0)
    for h in range(q.shape[1] // HEAD):
        q_ref[:, h * HEAD : (h + 1) * HEAD] = _turn(q[:, h * HEAD : (h + 1) * HEAD], cos, sin)
    kv = _dot(a, jnp.concatenate([wk_ref[...], wv_ref[...]], axis=1), 1, 0)
    k_ref[...] = _turn(kv[:, :HEAD], cos, sin)
    v_ref[...] = kv[:, HEAD:].astype(jnp.bfloat16)


def qkv(a, wq, wk, wv, cos, sin, tile=256):
    rows, depth = a.shape
    row = lambda n: pl.BlockSpec((tile, n), lambda i: (i, 0))
    wide = wq.shape[1]
    return pl.pallas_call(
        _qkv_kernel,
        grid=(rows // tile,),
        in_specs=[row(depth), _whole(wq.shape), _whole(wk.shape), _whole(wv.shape), row(HEAD), row(HEAD)],
        out_specs=[row(wide), row(HEAD), row(HEAD)],
        out_shape=[_like((rows, wide)), _like((rows, HEAD)), _like((rows, HEAD))],
        compiler_params=_params(),
        cost_estimate=_cost(2 * rows * depth * (wide + 2 * HEAD), [a, wq, wk, wv]),
        name="qkv",
    )(a, wq, wk, wv, cos, sin)


def _nt_kernel(a_ref, w_ref, o_ref):
    o_ref[...] = _dot(a_ref[...], w_ref[...], 1, 1).astype(jnp.bfloat16)


def back_through_wo(dy, wo, tile=512):
    rows, depth = dy.shape
    return pl.pallas_call(
        _nt_kernel,
        grid=(rows // tile,),
        in_specs=[pl.BlockSpec((tile, depth), lambda i: (i, 0)), _whole(wo.shape)],
        out_specs=pl.BlockSpec((tile, wo.shape[0]), lambda i: (i, 0)),
        out_shape=_like((rows, wo.shape[0])),
        compiler_params=_params(),
        cost_estimate=_cost(2 * rows * depth * wo.shape[0], [dy, wo]),
        name="back_through_wo",
    )(dy, wo)


def _gaps(bk, span, block, start):
    column = lax.broadcasted_iota(jnp.int32, (bk, DEVS * span), 1)
    place = (column // span) * block + start + column % span
    return place - lax.broadcasted_iota(jnp.int32, (bk, DEVS * span), 0)


def _edge(span, block, start):
    return -(-((DEVS - 1) * block + start + span) // 128) * 128


def _forward(q_ref, k_ref, v_ref, o_ref, lse_ref, top_s, mix_s, gap_s, *, span, block, start):
    p = pl.program_id(0)
    nq = DEVS * span
    heads = q_ref.shape[-1] // HEAD
    scale = HEAD**-0.5
    e = scale * LOG2E
    edge = _edge(span, block, start)

    @pl.when(p == 0)
    def _():
        gap_s[...] = _gaps(edge, span, block, start)

    top_s[...] = jnp.full(top_s.shape, NEG, jnp.float32)
    mix_s[...] = jnp.zeros(mix_s.shape, jnp.float32)

    def step(first, n, masked):
        here = pl.ds(first, n)
        k = k_ref[here, :]
        values = jnp.concatenate([v_ref[here, :].T, jnp.ones((8, n), jnp.bfloat16)], axis=0)
        scores = [_dot(k, q_ref[:, h * HEAD : (h + 1) * HEAD], 1, 1) for h in range(heads)]
        weights, keeps = [], []
        for h, s in enumerate(scores):
            if masked:
                s = jnp.where(gap_s[...] >= 0, s, HIDDEN)
            old = top_s[h : h + 1, :]
            top = jnp.maximum(old, s.max(axis=0, keepdims=True))
            top_s[h : h + 1, :] = top
            weights.append(jnp.exp2((s - top) * e).astype(jnp.bfloat16))
            keeps.append(jnp.exp2((old - top) * e))
        for h in range(heads):
            mix_s[h] = mix_s[h] * keeps[h] + _dot(values, weights[h], 1, 0)

    lax.fori_loop(0, p, lambda j, _: step(j * BK, BK, False), None)
    step(p * BK, edge, True)
    for h in range(heads):
        total = mix_s[h, HEAD : HEAD + 1, :]
        o_ref[:, h * HEAD : (h + 1) * HEAD] = (mix_s[h, :HEAD, :] * (1 / total)).T.astype(jnp.bfloat16)
        lse_ref[h : h + 1, :] = top_s[h : h + 1, :] * scale + jnp.log(total)


def attend(q, k, v, span, block, start):
    rows, wide = q.shape
    heads = wide // HEAD
    nq = DEVS * span
    edge = _edge(span, block, start)
    row = pl.BlockSpec((nq, wide), lambda i: (i, 0))
    return pl.pallas_call(
        functools.partial(_forward, span=span, block=block, start=start),
        grid=(rows // nq,),
        in_specs=[row, _whole(k.shape), _whole(v.shape)],
        out_specs=[row, pl.BlockSpec((heads, nq), lambda i: (0, i))],
        out_shape=[_like((rows, wide)), _like((heads, rows), jnp.float32)],
        scratch_shapes=[pltpu.VMEM((heads, nq), jnp.float32), pltpu.VMEM((heads, HEAD + 8, nq), jnp.float32), pltpu.VMEM((edge, nq), jnp.int32)],
        compiler_params=_params(),
        cost_estimate=_cost(2 * rows * wide * k.shape[0] * 2, [q, k, v, q], rows * heads * k.shape[0]),
        name="attend",
    )(q, k, v)


def _backward(*refs, span, block, start, carried, last):
    if carried:
        q_ref, k_ref, v_ref, do_ref, o_ref, lse_ref, cos_ref, sin_ref, dk_in, dv_in, *refs = refs
    else:
        q_ref, k_ref, v_ref, do_ref, o_ref, lse_ref, cos_ref, sin_ref, *refs = refs
    if last:
        kcos_ref, ksin_ref, *refs = refs
    dq_ref, dk_ref, dv_ref, dq_s, dk_s, dv_s, gap_s = refs
    p = pl.program_id(0)
    heads = q_ref.shape[-1] // HEAD
    scale = HEAD**-0.5
    e = scale * LOG2E
    edge = _edge(span, block, start)

    @pl.when(p == 0)
    def _():
        gap_s[...] = _gaps(edge, span, block, start)
        dk_s[...] = dk_in[...] if carried else jnp.zeros(dk_s.shape, jnp.float32)
        dv_s[...] = dv_in[...] if carried else jnp.zeros(dv_s.shape, jnp.float32)

    dq_s[...] = jnp.zeros(dq_s.shape, jnp.float32)
    head = lambda ref, h: ref[:, h * HEAD : (h + 1) * HEAD]
    lses = [lse_ref[h : h + 1, :] * LOG2E for h in range(heads)]
    deltas = [(head(do_ref, h).astype(jnp.float32) * head(o_ref, h).astype(jnp.float32)).T.sum(axis=0, keepdims=True) for h in range(heads)]

    def step(first, n, masked):
        here = pl.ds(first, n)
        k, v = k_ref[here, :], v_ref[here, :]
        kt = k.T
        scores = [_dot(k, head(q_ref, h), 1, 1) for h in range(heads)]
        dps = [_dot(v, head(do_ref, h), 1, 1) for h in range(heads)]
        for h in range(heads):
            w = jnp.exp2(scores[h] * e - lses[h])
            if masked:
                w = jnp.where(gap_s[...] >= 0, w, 0.0)
            ds = (w * (dps[h] - deltas[h])).astype(jnp.bfloat16)
            dv_s[here, :] += _dot(w.astype(jnp.bfloat16), head(do_ref, h), 1, 0)
            dk_s[here, :] += _dot(ds, head(q_ref, h), 1, 0)
            dq_s[h] += _dot(kt, ds, 1, 0)

    lax.fori_loop(0, p, lambda j, _: step(j * BK, BK, False), None)
    step(p * BK, edge, True)
    for h in range(heads):
        dq_ref[:, h * HEAD : (h + 1) * HEAD] = _turn((dq_s[h] * scale).T, cos_ref[...], -sin_ref[...])

    @pl.when(p == pl.num_programs(0) - 1)
    def _():
        if last:
            dk_ref[...] = _turn(dk_s[...] * scale, kcos_ref[...], -ksin_ref[...])
            dv_ref[...] = dv_s[...].astype(jnp.bfloat16)
        else:
            dk_ref[...] = dk_s[...]
            dv_ref[...] = dv_s[...]


def attend_bwd(q, k, v, d_out, out, lse, cos, sin, carry, turn, span, block, start):
    rows, wide = q.shape
    heads = wide // HEAD
    nq = DEVS * span
    keys = k.shape[0]
    edge = _edge(span, block, start)
    row = pl.BlockSpec((nq, wide), lambda i: (i, 0))
    table = pl.BlockSpec((nq, HEAD), lambda i: (i, 0))
    kv = _whole(k.shape)
    more = [*(carry or ()), *(turn or ())]
    to = jnp.float32 if turn is None else jnp.bfloat16
    return pl.pallas_call(
        functools.partial(_backward, span=span, block=block, start=start, carried=carry is not None, last=turn is not None),
        grid=(rows // nq,),
        in_specs=[row, kv, kv, row, row, pl.BlockSpec((heads, nq), lambda i: (0, i)), table, table] + [kv] * len(more),
        out_specs=[row, pl.BlockSpec(k.shape, lambda i: (0, 0)), pl.BlockSpec(k.shape, lambda i: (0, 0))],
        out_shape=[_like((rows, wide)), _like(k.shape, to), _like(k.shape, to)],
        scratch_shapes=[pltpu.VMEM((heads, HEAD, nq), jnp.float32), pltpu.VMEM((keys, HEAD), jnp.float32),
                        pltpu.VMEM((keys, HEAD), jnp.float32), pltpu.VMEM((edge, nq), jnp.int32)],
        compiler_params=_params(),
        cost_estimate=_cost(2 * rows * wide * keys * 5, [q, q, q, q, k, v, k, v], rows * heads * keys),
        name="attend_bwd",
    )(q, k, v, d_out, out, lse, cos, sin, *more)


def _fill(cat_s, dqs, dk_ref, dv_ref):
    wide = dqs[0].shape[1]
    rows = cat_s.shape[1]
    for n, dq in enumerate(dqs):
        cat_s[n, :, :wide] = dq[...]
        cat_s[n, :, wide : wide + HEAD] = dk_ref[:, n].reshape(rows, HEAD)
        cat_s[n, :, wide + HEAD :] = dv_ref[:, n].reshape(rows, HEAD)


def _da_kernel(*refs):
    dqs, (dk_ref, dv_ref, wq_ref, wk_ref, wv_ref, o_ref, cat_s) = refs[:PARTS], refs[PARTS:]

    @pl.when(pl.program_id(0) == 0)
    def _():
        _fill(cat_s, dqs, dk_ref, dv_ref)

    w = jnp.concatenate([wq_ref[...], wk_ref[...], wv_ref[...]], axis=1)
    for n in range(PARTS):
        got = _dot(cat_s[n], w, 1, 1)
        o_ref[:, n] = got.astype(jnp.bfloat16).reshape(o_ref.shape[0], o_ref.shape[2], -1)


def grad_a(dqs, dk, dv, wq, wk, wv, first, columns, tile=256):
    n, parts, span, _ = dk.shape
    wide = wq.shape[1]
    at = first // tile
    weights = lambda w: pl.BlockSpec((tile, w.shape[1]), lambda i: (i + at, 0))
    return pl.pallas_call(
        _da_kernel,
        grid=(columns // tile,),
        in_specs=[*(_whole(x.shape) for x in dqs), _whole(dk.shape), _whole(dv.shape), weights(wq), weights(wk), weights(wv)],
        out_specs=pl.BlockSpec((n, parts, span, tile), lambda i: (0, 0, 0, i)),
        out_shape=_like((n, parts, span, columns)),
        scratch_shapes=[pltpu.VMEM((parts, n * span, wide + 2 * HEAD), jnp.bfloat16)],
        compiler_params=_params(),
        cost_estimate=_cost(2 * n * parts * span * columns * (wide + 2 * HEAD), [*dqs, dk, dv]),
        name="grad_a",
    )(*dqs, dk, dv, wq, wk, wv)


def _dw_kernel(*refs):
    xs, dqs, (dk_ref, dv_ref, oq_ref, ok_ref, ov_ref, cat_s) = refs[:PARTS], refs[PARTS : 2 * PARTS], refs[2 * PARTS :]

    @pl.when(pl.program_id(0) == 0)
    def _():
        _fill(cat_s, dqs, dk_ref, dv_ref)

    got = _dot(xs[0][...], cat_s[0], 0, 0)
    for n in range(1, PARTS):
        got += _dot(xs[n][...], cat_s[n], 0, 0)
    wide = oq_ref.shape[1]
    oq_ref[...] = got[:, :wide].astype(jnp.bfloat16)
    ok_ref[...] = got[:, wide : wide + HEAD].astype(jnp.bfloat16)
    ov_ref[...] = got[:, wide + HEAD :].astype(jnp.bfloat16)


def grad_qkv(xs, dqs, dk, dv, tile=512):
    rows, depth = xs[0].shape
    wide = dqs[0].shape[1]
    out = lambda w: pl.BlockSpec((tile, w), lambda i: (i, 0))
    return pl.pallas_call(
        _dw_kernel,
        grid=(depth // tile,),
        in_specs=[*(pl.BlockSpec((rows, tile), lambda i: (0, i)) for _ in xs), *(_whole(x.shape) for x in dqs), _whole(dk.shape), _whole(dv.shape)],
        out_specs=[out(wide), out(HEAD), out(HEAD)],
        out_shape=[_like((depth, wide)), _like((depth, HEAD)), _like((depth, HEAD))],
        scratch_shapes=[pltpu.VMEM((PARTS, rows, wide + 2 * HEAD), jnp.bfloat16)],
        compiler_params=_params(),
        cost_estimate=_cost(2 * PARTS * rows * depth * (wide + 2 * HEAD), [*xs, *dqs, dk, dv]),
        name="grad_qkv",
    )(*xs, *dqs, dk, dv)


def _dwo_kernel(*refs):
    outs, dys, o_ref = refs[:PARTS], refs[PARTS : 2 * PARTS], refs[-1]
    got = _dot(outs[0][...], dys[0][...], 0, 0)
    for n in range(1, PARTS):
        got += _dot(outs[n][...], dys[n][...], 0, 0)
    o_ref[...] = got.astype(jnp.bfloat16)


def grad_wo(outs, dys, tile=512):
    rows, depth = dys[0].shape
    wide = outs[0].shape[1]
    return pl.pallas_call(
        _dwo_kernel,
        grid=(depth // tile,),
        in_specs=[*(_whole(x.shape) for x in outs), *(pl.BlockSpec((rows, tile), lambda i: (0, i)) for _ in dys)],
        out_specs=pl.BlockSpec((wide, tile), lambda i: (0, i)),
        out_shape=_like((wide, depth)),
        compiler_params=_params(),
        cost_estimate=_cost(2 * PARTS * rows * depth * wide, [*outs, *dys]),
        name="grad_wo",
    )(*outs, *dys)


def _norm_kernel(*refs):
    x_ref, dy_ref, gain_ref, *das, o_ref, og_ref = refs
    x = x_ref[...].astype(jnp.float32)
    scale = lax.rsqrt(jnp.mean(x * x, -1, keepdims=True) + 1e-6)
    da = jnp.concatenate([r[...].astype(jnp.float32) for r in das], axis=1)
    unit = x * scale
    by_unit = da * gain_ref[...].astype(jnp.float32)
    mean = jnp.mean(by_unit * unit, -1, keepdims=True)
    o_ref[...] = (dy_ref[...].astype(jnp.float32) + scale * (by_unit - unit * mean)).astype(jnp.bfloat16)
    part = jnp.sum(da * unit, axis=0, keepdims=True)

    @pl.when(pl.program_id(0) == 0)
    def _():
        og_ref[...] = part

    @pl.when(pl.program_id(0) > 0)
    def _():
        og_ref[...] += part


def norm_bwd(x, dy, gain, das, tile=32):
    rows, depth = x.shape
    row = lambda n: pl.BlockSpec((tile, n), lambda i: (i, 0))
    return pl.pallas_call(
        _norm_kernel,
        grid=(rows // tile,),
        in_specs=[row(depth), row(depth), _whole((1, depth)), *(row(d.shape[1]) for d in das)],
        out_specs=[row(depth), pl.BlockSpec((1, depth), lambda i: (0, 0))],
        out_shape=[_like((rows, depth)), _like((1, depth), jnp.float32)],
        compiler_params=_params(),
        cost_estimate=_cost(20 * rows * depth, [x, dy, x, x]),
        name="norm_bwd",
    )(x, dy, gain.reshape(1, depth), *das)


def _share_kernel(n, mine_ref, o_ref, held, send_sem, recv_sem):
    me = lax.axis_index("tp")
    barrier = pltpu.get_barrier_semaphore()
    for d in range(1, n):
        pl.semaphore_signal(barrier, inc=1, device_id={"tp": lax.rem(me + d, n)}, device_id_type=pl.DeviceIdType.MESH)
    pl.semaphore_wait(barrier, n - 1)
    copies = []
    for d in range(1, n):
        copy = pltpu.make_async_remote_copy(src_ref=mine_ref, dst_ref=held.at[d - 1], send_sem=send_sem.at[d - 1], recv_sem=recv_sem.at[d - 1],
                                            device_id={"tp": lax.rem(me + d, n)}, device_id_type=pl.DeviceIdType.MESH)
        copy.start()
        copies.append(copy)
    for copy in copies:
        copy.wait()
    total = jnp.zeros(o_ref.shape, jnp.float32)
    for i in range(n):
        other = held[jnp.maximum(lax.rem(me - i + n, n) - 1, 0)]
        total += jnp.where(me == i, mine_ref[...], other)
    o_ref[...] = total


def share_sum(part, n):
    depth = part.shape[1]
    wide = part.reshape(8, depth // 8)
    return pl.pallas_call(
        functools.partial(_share_kernel, n),
        in_specs=[pl.BlockSpec(memory_space=pltpu.VMEM)],
        out_specs=pl.BlockSpec(memory_space=pltpu.VMEM),
        out_shape=_like(wide.shape, jnp.float32),
        scratch_shapes=[pltpu.VMEM((n - 1, *wide.shape), jnp.float32), pltpu.SemaphoreType.DMA((n - 1,)), pltpu.SemaphoreType.DMA((n - 1,))],
        compiler_params=pltpu.CompilerParams(collective_id=0, has_side_effects=True),
        cost_estimate=pl.CostEstimate(flops=n * depth, transcendentals=0, bytes_accessed=8 * depth),
        name="share_sum",
    )(wide).reshape(1, depth)


def solution(mesh):
    n = mesh.shape["tp"]

    def step(x, dy, gain, wq, wk, wv, wo):
        block, depth = x.shape
        rows = n * block
        span = block // PARTS

        def gather(t, name):
            with jax.named_scope(name):
                return lax.all_gather(t, "tp", axis=0, tiled=True)

        half = HEAD // 2
        angle = jnp.arange(rows, dtype=jnp.float32)[:, None] * THETA ** (-jnp.arange(half, dtype=jnp.float32) / half)
        cos, sin = jnp.cos(angle), jnp.sin(angle)
        cos, sin = jnp.concatenate([cos, cos], 1), jnp.concatenate([-sin, sin], 1)
        part = lambda t, s: t.reshape(n, PARTS, span, -1)[:, s].reshape(n * span, -1)
        coss, sins = [part(cos, s) for s in range(PARTS)], [part(sin, s) for s in range(PARTS)]

        a = normed(x, gain)
        xs = [gather(a[s * span : (s + 1) * span], f"ag_a{s}") for s in range(PARTS)]
        dys = [gather(dy[s * span : (s + 1) * span], f"ag_dy{s}") for s in range(PARTS)]
        got = [qkv(xs[s], wq, wk, wv, coss[s], sins[s]) for s in range(PARTS)]
        q = [g[0] for g in got]
        whole = lambda i: jnp.stack([g[i].reshape(n, span, HEAD) for g in got], 1).reshape(rows, HEAD)
        k, v = whole(1), whole(2)
        seen = [attend(q[s], k, v, span, block, s * span) for s in range(PARTS)]
        dqs, carry = [], None
        for s in range(PARTS):
            d_out = back_through_wo(dys[s], wo)
            dq, *carry = attend_bwd(q[s], k, v, d_out, *seen[s], coss[s], sins[s], carry, (cos, sin) if s == PARTS - 1 else None, span, block, s * span)
            dqs.append(dq)
        dk, dv = (t.reshape(n, PARTS, span, HEAD) for t in carry)
        width = depth // COLS
        das = []
        for c in range(COLS):
            term = grad_a(dqs, dk, dv, wq, wk, wv, c * width, width).reshape(rows, width)
            with jax.named_scope(f"rs{c}"):
                das.append(lax.psum_scatter(term, "tp", scatter_dimension=0, tiled=True))
        by_wo = grad_wo([o for o, _ in seen], dys)
        by_wq, by_wk, by_wv = grad_qkv(xs, dqs, dk, dv)
        by_x, by_gain = norm_bwd(x, dy, gain, das)
        return by_x, share_sum(by_gain, n), by_wq, by_wk, by_wv, by_wo

    tokens, columns = P(("dp", "tp"), None), P(None, "tp")
    return jax.shard_map(
        step,
        mesh=mesh,
        in_specs=(tokens, tokens, P(None), columns, columns, columns, P("tp", None)),
        out_specs=(tokens, P("dp", None), P("dp", "tp"), P("dp", "tp"), P("dp", "tp"), P(("dp", "tp"), None)),
        check_vma=False,
    )
```

```python
import functools

import jax
import jax.numpy as jnp
from jax import lax
from jax.experimental import pallas as pl
from jax.experimental.pallas import tpu as pltpu
from jax.sharding import PartitionSpec as P


NEG = -1e30
HIDDEN = 2 * NEG
LOG2E = 1.4426950408889634
VMEM = 62 * 2**20
HEAD = 128
THETA = 10000
PARTS = 2
DEVS = 2
BK = 512
WO_STEPS = (0, 4), (4, 10)
QKV_STEPS = (0, 14), (14, 14)
PIECES = 2


def _dot(a, b, ca, cb):
    return lax.dot_general(a, b, (((ca,), (cb,)), ((), ())), preferred_element_type=jnp.float32)


def _whole(shape):
    return pl.BlockSpec(shape, lambda *_: (0,) * len(shape), pipeline_mode=pl.Buffered(1))


def _params(n=1):
    return pltpu.CompilerParams(dimension_semantics=("arbitrary",) * n, vmem_limit_bytes=VMEM)


def _cost(flops, arrays, exps=0):
    return pl.CostEstimate(flops=int(flops), transcendentals=int(exps), bytes_accessed=sum(a.size * a.dtype.itemsize for a in arrays))


def _like(shape, dtype=jnp.bfloat16):
    return jax.ShapeDtypeStruct(shape, dtype)


def _normed_kernel(x_ref, gain_ref, o_ref):
    wide = x_ref[...].astype(jnp.float32)
    scale = lax.rsqrt(jnp.mean(wide * wide, -1, keepdims=True) + 1e-6)
    o_ref[...] = (wide * scale * gain_ref[...].astype(jnp.float32)).astype(jnp.bfloat16)


def normed(x, gain, tile=64):
    rows, depth = x.shape
    row = pl.BlockSpec((tile, depth), lambda i: (i, 0))
    return pl.pallas_call(
        _normed_kernel,
        grid=(rows // tile,),
        in_specs=[row, _whole((1, depth))],
        out_specs=row,
        out_shape=_like((rows, depth)),
        compiler_params=_params(),
        cost_estimate=_cost(6 * rows * depth, [x, x]),
        name="normed",
    )(x, gain.reshape(1, depth))


def _turn(t, cos, sin):
    t = t.astype(jnp.bfloat16).astype(jnp.float32)
    return (t * cos + pltpu.roll(t, HEAD // 2, 1) * sin).astype(jnp.bfloat16)


def _qkv_kernel(a_ref, w_ref, cos_ref, sin_ref, q_ref, k_ref, v_ref, acc, *, wide, some):
    i = pl.program_id(0)

    @pl.loop(0, a_ref.shape[0] // some)
    def _(r):
        at = pl.ds(r * some, some)
        got = _dot(a_ref[at, :], w_ref[...], 1, 0)

        @pl.when(i == 0)
        def _():
            acc[at, :] = got

        @pl.when(i > 0)
        def _():
            acc[at, :] += got

    @pl.when(i == pl.num_programs(0) - 1)
    def _():
        @pl.loop(0, a_ref.shape[0] // HEAD)
        def _(r):
            at = pl.ds(r * HEAD, HEAD)
            cos, sin = cos_ref[at, :], sin_ref[at, :]
            for h in range(0, wide, HEAD):
                q_ref[at, h : h + HEAD] = _turn(acc[at, h : h + HEAD], cos, sin)
            k_ref[at, :] = _turn(acc[at, wide : wide + HEAD], cos, sin)
            v_ref[at, :] = acc[at, wide + HEAD :].astype(jnp.bfloat16)


def qkv(a, w, cos, sin, tile=512, some=512):
    rows, depth = a.shape
    total = w.shape[1]
    wide = total - 2 * HEAD
    return pl.pallas_call(
        functools.partial(_qkv_kernel, wide=wide, some=some),
        grid=(depth // tile,),
        in_specs=[pl.BlockSpec((rows, tile), lambda i: (0, i)), pl.BlockSpec((tile, total), lambda i: (i, 0)), _whole(cos.shape), _whole(sin.shape)],
        out_specs=[_whole((rows, wide)), _whole((rows, HEAD)), _whole((rows, HEAD))],
        out_shape=[_like((rows, wide)), _like((rows, HEAD)), _like((rows, HEAD))],
        scratch_shapes=[pltpu.VMEM((rows, total), jnp.float32)],
        compiler_params=_params(),
        cost_estimate=_cost(2 * rows * depth * total, [a, w]),
        name="qkv",
    )(a, w, cos, sin)


def _wo_kernel(a_ref, w_ref, o_ref, acc, *, some):
    i = pl.program_id(0)

    @pl.loop(0, a_ref.shape[0] // some)
    def _(r):
        at = pl.ds(r * some, some)
        got = _dot(a_ref[at, :], w_ref[...], 1, 1)

        @pl.when(i == 0)
        def _():
            acc[at, :] = got

        @pl.when(i > 0)
        def _():
            acc[at, :] += got

        @pl.when(i == pl.num_programs(0) - 1)
        def _():
            o_ref[at, :] = acc[at, :].astype(jnp.bfloat16)


def back_through_wo(dy, wo, tile=1024, some=512):
    rows, depth = dy.shape
    wide = wo.shape[0]
    return pl.pallas_call(
        functools.partial(_wo_kernel, some=some),
        grid=(depth // tile,),
        in_specs=[pl.BlockSpec((rows, tile), lambda i: (0, i)), pl.BlockSpec((wide, tile), lambda i: (0, i))],
        out_specs=_whole((rows, wide)),
        out_shape=_like((rows, wide)),
        scratch_shapes=[pltpu.VMEM((rows, wide), jnp.float32)],
        compiler_params=_params(),
        cost_estimate=_cost(2 * rows * depth * wide, [dy, wo]),
        name="back_through_wo",
    )(dy, wo)


def _gaps(bk, span, block, start):
    column = lax.broadcasted_iota(jnp.int32, (bk, DEVS * span), 1)
    place = (column // span) * block + start + column % span
    return place - lax.broadcasted_iota(jnp.int32, (bk, DEVS * span), 0)


def _edge(span, block, start):
    return -(-((DEVS - 1) * block + start + span) // 128) * 128


def _forward(q_ref, k_ref, v_ref, o_ref, lse_ref, top_s, mix_s, gap_s, *, span, block, start):
    p = pl.program_id(0)
    heads = q_ref.shape[-1] // HEAD
    scale = HEAD**-0.5
    e = scale * LOG2E
    edge = _edge(span, block, start)
    head = lambda ref, h: ref[:, 0, :, h * HEAD : (h + 1) * HEAD].reshape(-1, HEAD)

    @pl.when(p == 0)
    def _():
        gap_s[...] = _gaps(edge, span, block, start)

    top_s[...] = jnp.full(top_s.shape, NEG, jnp.float32)
    mix_s[...] = jnp.zeros(mix_s.shape, jnp.float32)

    def step(first, n, masked):
        here = pl.ds(first, n)
        k = k_ref[here, :]
        values = jnp.concatenate([v_ref[here, :].T, jnp.ones((8, n), jnp.bfloat16)], axis=0)
        scores = [_dot(k, head(q_ref, h), 1, 1) for h in range(heads)]
        weights, keeps = [], []
        for h, s in enumerate(scores):
            if masked:
                s = jnp.where(gap_s[...] >= 0, s, HIDDEN)
            old = top_s[h : h + 1, :]
            top = jnp.maximum(old, s.max(axis=0, keepdims=True))
            top_s[h : h + 1, :] = top
            weights.append(jnp.exp2((s - top) * e).astype(jnp.bfloat16))
            keeps.append(jnp.exp2((old - top) * e))
        for h in range(heads):
            mix_s[h] = mix_s[h] * keeps[h] + _dot(values, weights[h], 1, 0)

    lax.fori_loop(0, p, lambda j, _: step(j * BK, BK, False), None)
    step(p * BK, edge, True)
    for h in range(heads):
        total = mix_s[h, HEAD : HEAD + 1, :]
        o_ref[:, h * HEAD : (h + 1) * HEAD] = (mix_s[h, :HEAD, :] * (1 / total)).T.astype(jnp.bfloat16)
        lse_ref[h : h + 1, :] = top_s[h : h + 1, :] * scale + jnp.log(total)


def attend(q, k, v, span, block, start):
    devices, _, _, wide = q.shape
    rows = devices * span
    heads = wide // HEAD
    nq = DEVS * span
    edge = _edge(span, block, start)
    row = pl.BlockSpec((nq, wide), lambda i: (i, 0))
    part = pl.BlockSpec((DEVS, 1, span, wide), lambda i: (i, start // span, 0, 0))
    return pl.pallas_call(
        functools.partial(_forward, span=span, block=block, start=start),
        grid=(rows // nq,),
        in_specs=[part, _whole(k.shape), _whole(v.shape)],
        out_specs=[row, pl.BlockSpec((heads, nq), lambda i: (0, i))],
        out_shape=[_like((rows, wide)), _like((heads, rows), jnp.float32)],
        scratch_shapes=[pltpu.VMEM((heads, nq), jnp.float32), pltpu.VMEM((heads, HEAD + 8, nq), jnp.float32), pltpu.VMEM((edge, nq), jnp.int32)],
        compiler_params=_params(),
        cost_estimate=_cost(2 * rows * wide * k.shape[0] * 2, [q, k, v], rows * heads * k.shape[0]),
        name="attend",
    )(q, k, v)


def _backward(*refs, span, block, start, carried, last):
    q_ref, k_ref, v_ref, do_ref, o_ref, lse_ref, cos_ref, sin_ref, *refs = refs
    if carried:
        dk_in, dv_in, *refs = refs
    if last:
        kcos_ref, ksin_ref, dq_ref, dkv_ref, *refs = refs
    else:
        dq_ref, dk_ref, dv_ref, *refs = refs
    dq_s, dk_s, dv_s, gap_s = refs
    p = pl.program_id(0)
    heads = q_ref.shape[-1] // HEAD
    scale = HEAD**-0.5
    e = scale * LOG2E
    edge = _edge(span, block, start)

    @pl.when(p == 0)
    def _():
        gap_s[...] = _gaps(edge, span, block, start)
        dk_s[...] = dk_in[...] if carried else jnp.zeros(dk_s.shape, jnp.float32)
        dv_s[...] = dv_in[...] if carried else jnp.zeros(dv_s.shape, jnp.float32)

    dq_s[...] = jnp.zeros(dq_s.shape, jnp.float32)
    part = lambda ref, h: ref[:, 0, :, h * HEAD : (h + 1) * HEAD].reshape(-1, HEAD)
    head = lambda ref, h: ref[:, h * HEAD : (h + 1) * HEAD]
    lses = [lse_ref[h : h + 1, :] * LOG2E for h in range(heads)]
    deltas = [(head(do_ref, h).astype(jnp.float32) * head(o_ref, h).astype(jnp.float32)).T.sum(axis=0, keepdims=True) for h in range(heads)]

    def step(first, n, masked):
        here = pl.ds(first, n)
        k, v = k_ref[here, :], v_ref[here, :]
        kt = k.T
        scores = [_dot(k, part(q_ref, h), 1, 1) for h in range(heads)]
        dps = [_dot(v, head(do_ref, h), 1, 1) for h in range(heads)]
        for h in range(heads):
            w = jnp.exp2(scores[h] * e - lses[h])
            if masked:
                w = jnp.where(gap_s[...] >= 0, w, 0.0)
            ds = (w * (dps[h] - deltas[h])).astype(jnp.bfloat16)
            dv_s[here, :] += _dot(w.astype(jnp.bfloat16), head(do_ref, h), 1, 0)
            dk_s[here, :] += _dot(ds, part(q_ref, h), 1, 0)
            dq_s[h] += _dot(kt, ds, 1, 0)

    lax.fori_loop(0, p, lambda j, _: step(j * BK, BK, False), None)
    step(p * BK, edge, True)
    cos, sin = (r[:, 0].reshape(-1, HEAD) for r in (cos_ref, sin_ref))
    for h in range(heads):
        dq_ref[:, 0, :, h * HEAD : (h + 1) * HEAD] = _turn((dq_s[h] * scale).T, cos, -sin).reshape(DEVS, span, HEAD)

    @pl.when(p == pl.num_programs(0) - 1)
    def _():
        if last:
            dkv_ref[:, :HEAD] = _turn(dk_s[...] * scale, kcos_ref[...], -ksin_ref[...])
            dkv_ref[:, HEAD:] = dv_s[...].astype(jnp.bfloat16)
        else:
            dk_ref[...] = dk_s[...]
            dv_ref[...] = dv_s[...]


def attend_bwd(q, k, v, d_out, out, lse, cos, sin, carry, last, span, block, start):
    devices, _, _, wide = q.shape
    rows = devices * span
    heads = wide // HEAD
    nq = DEVS * span
    keys = k.shape[0]
    edge = _edge(span, block, start)
    row = pl.BlockSpec((nq, wide), lambda i: (i, 0))
    part = lambda w: pl.BlockSpec((DEVS, 1, span, w), lambda i: (i, start // span, 0, 0))
    kv = _whole(k.shape)
    more = [*(carry or ()), *((cos, sin) if last else ())]
    tables = [t.reshape(devices, -1, span, HEAD) for t in (cos, sin)]
    sums = [(keys, 2 * HEAD)] if last else [k.shape, k.shape]
    return pl.pallas_call(
        functools.partial(_backward, span=span, block=block, start=start, carried=carry is not None, last=last),
        grid=(rows // nq,),
        in_specs=[part(wide), kv, kv, row, row, pl.BlockSpec((heads, nq), lambda i: (0, i)), part(HEAD), part(HEAD)] + [kv] * len(more),
        out_specs=[pl.BlockSpec((DEVS, 1, span, wide), lambda i: (0, i, 0, 0)), *(_whole(t) for t in sums)],
        out_shape=[_like((DEVS, devices // DEVS, span, wide)), *(_like(t, jnp.bfloat16 if last else jnp.float32) for t in sums)],
        scratch_shapes=[pltpu.VMEM((heads, HEAD, nq), jnp.float32), pltpu.VMEM((keys, HEAD), jnp.float32),
                        pltpu.VMEM((keys, HEAD), jnp.float32), pltpu.VMEM((edge, nq), jnp.int32)],
        compiler_params=_params(),
        cost_estimate=_cost(2 * rows * wide * keys * 5, [d_out, out, k, v, k, v], rows * heads * keys),
        name="attend_bwd",
    )(q, k, v, d_out, out, lse, *tables, *more)


def _da_kernel(at_ref, *refs, parts, more):
    dqs, refs = refs[:parts], refs[parts:]
    dkv_ref, *refs = refs
    pqs, refs = refs[:parts], refs[parts:]
    pkv_ref, w_ref, pw_ref, *refs = refs
    if more:
        sum_ref, *refs = refs
    o_ref, mine_s, other_s = refs
    wide = dqs[0].shape[-1]
    span = dqs[0].shape[-2]

    @pl.when(pl.program_id(0) == 0)
    def _():
        for n in range(parts):
            mine_s[n * span : (n + 1) * span, :wide] = dqs[n][0, 0]
            other_s[n * span : (n + 1) * span, :wide] = pqs[n][0]
        mine_s[:, wide:] = dkv_ref[0, 0]
        other_s[:, wide:] = pkv_ref[0]

    got = _dot(mine_s[...], w_ref[...], 1, 1) + _dot(other_s[...], pw_ref[...], 1, 1)
    if more:
        got += sum_ref[...].astype(jnp.float32)
    o_ref[...] = got.astype(jnp.bfloat16)


def grad_a(table, row, dqs, dkv, pqs, pkv, w, pw, total, first, columns, tile=256):
    wide = dqs[0].shape[-1]
    span = dqs[0].shape[-2]
    rows = len(dqs) * span
    depth = w.shape[1]
    skip = first // tile
    weights = pl.BlockSpec((tile, depth), lambda i, at: (i + skip, 0))
    out = pl.BlockSpec((rows, tile), lambda i, at: (0, i))
    return pl.pallas_call(
        functools.partial(_da_kernel, parts=len(dqs), more=total is not None),
        grid_spec=pltpu.PrefetchScalarGridSpec(
            num_scalar_prefetch=1,
            grid=(columns // tile,),
            in_specs=[*(pl.BlockSpec((1, 1, span, wide), lambda i, at: (at[row, 0], at[row, 1], 0, 0)) for _ in dqs),
                      pl.BlockSpec((1, 1, rows, 2 * HEAD), lambda i, at: (at[row, 1], at[row, 0], 0, 0)),
                      *(pl.BlockSpec((1, span, wide), lambda i, at: (at[row, 1], 0, 0)) for _ in pqs),
                      pl.BlockSpec((1, rows, 2 * HEAD), lambda i, at: (at[row, 1], 0, 0)), weights, weights] + ([] if total is None else [out]),
            out_specs=out,
            scratch_shapes=[pltpu.VMEM((rows, depth), jnp.bfloat16), pltpu.VMEM((rows, depth), jnp.bfloat16)],
        ),
        out_shape=_like((rows, columns)),
        compiler_params=_params(),
        cost_estimate=pl.CostEstimate(flops=4 * rows * columns * depth, transcendentals=0, bytes_accessed=4 * columns * depth),
        name="grad_a",
    )(table, *dqs, dkv, *pqs, pkv, w, pw, *(() if total is None else (total,)))


def _dw_kernel(*refs, parts, span):
    x_ref, *refs = refs
    dqs, refs = refs[:parts], refs[parts:]
    dkv_ref, *refs = refs
    oq_ref, ok_ref, ov_ref, cat_s = refs[-4:]
    wide = oq_ref.shape[1]

    @pl.when(pl.program_id(0) == 0)
    def _():
        cat_s[:, wide:] = dkv_ref[...]
        cores, chips = dqs[0].shape[:2]
        for chip in range(chips):
            for core in range(cores):
                for n in range(parts):
                    at = ((chip * cores + core) * parts + n) * span
                    cat_s[at : at + span, :wide] = dqs[n][core, chip]

    got = _dot(x_ref[...], cat_s[...], 0, 0)
    oq_ref[...] = got[:, :wide].astype(jnp.bfloat16)
    ok_ref[...] = got[:, wide : wide + HEAD].astype(jnp.bfloat16)
    ov_ref[...] = got[:, wide + HEAD :].astype(jnp.bfloat16)


def grad_qkv(x, dqs, dkv, sofar, skip, steps, tile=256):
    rows, depth = x.shape
    wide = dqs[0].shape[-1]
    shapes = [(depth, wide), (depth, HEAD), (depth, HEAD)]
    given = [x, *dqs, dkv]
    sofar = sofar or ()
    return pl.pallas_call(
        functools.partial(_dw_kernel, parts=len(dqs), span=dqs[0].shape[-2]),
        grid=(steps,),
        in_specs=[pl.BlockSpec((rows, tile), lambda i: (0, i + skip)), *(_whole(t.shape) for t in given[1:]), *(pl.BlockSpec(memory_space=pl.ANY) for _ in sofar)],
        out_specs=[pl.BlockSpec((tile, t[1]), lambda i: (i + skip, 0)) for t in shapes],
        out_shape=[_like(t) for t in shapes],
        scratch_shapes=[pltpu.VMEM((rows, wide + 2 * HEAD), jnp.bfloat16)],
        input_output_aliases={len(given) + n: n for n in range(len(sofar))},
        compiler_params=_params(),
        cost_estimate=pl.CostEstimate(flops=2 * rows * steps * tile * (wide + 2 * HEAD), transcendentals=0, bytes_accessed=2 * steps * tile * rows),
        name="grad_qkv",
    )(*given, *sofar)


def _dwo_kernel(*refs, parts):
    outs, dys, o_ref = refs[:parts], refs[parts : 2 * parts], refs[-1]
    got = _dot(outs[0][...], dys[0][...], 0, 0)
    for n in range(1, parts):
        got += _dot(outs[n][...], dys[n][...], 0, 0)
    o_ref[...] = got.astype(jnp.bfloat16)


def grad_wo(outs, dys, sofar, skip, steps, tile=512):
    rows, depth = dys[0].shape
    wide = outs[0].shape[1]
    given = [*outs, *dys]
    sofar = [] if sofar is None else [sofar]
    return pl.pallas_call(
        functools.partial(_dwo_kernel, parts=len(outs)),
        grid=(steps,),
        in_specs=[*(_whole(x.shape) for x in outs), *(pl.BlockSpec((rows, tile), lambda i: (0, i + skip)) for _ in dys), *(pl.BlockSpec(memory_space=pl.ANY) for _ in sofar)],
        out_specs=pl.BlockSpec((wide, tile), lambda i: (0, i + skip)),
        out_shape=_like((wide, depth)),
        input_output_aliases={len(given): 0} if sofar else {},
        compiler_params=_params(),
        cost_estimate=pl.CostEstimate(flops=2 * len(outs) * rows * steps * tile * wide, transcendentals=0, bytes_accessed=4 * steps * tile * rows),
        name="grad_wo",
    )(*given, *sofar)


def _norm_kernel(*refs):
    x_ref, dy_ref, gain_ref, *das, o_ref, og_ref = refs
    x = x_ref[...].astype(jnp.float32)
    scale = lax.rsqrt(jnp.mean(x * x, -1, keepdims=True) + 1e-6)
    da = jnp.concatenate([r[...].astype(jnp.float32) for r in das], axis=1)
    unit = x * scale
    by_unit = da * gain_ref[...].astype(jnp.float32)
    mean = jnp.mean(by_unit * unit, -1, keepdims=True)
    o_ref[...] = (dy_ref[...].astype(jnp.float32) + scale * (by_unit - unit * mean)).astype(jnp.bfloat16)
    part = jnp.sum(da * unit, axis=0, keepdims=True)

    @pl.when(pl.program_id(0) == 0)
    def _():
        og_ref[...] = part

    @pl.when(pl.program_id(0) > 0)
    def _():
        og_ref[...] += part


def norm_bwd(x, dy, gain, das, tile=32):
    rows, depth = x.shape
    row = lambda n: pl.BlockSpec((tile, n), lambda i: (i, 0))
    return pl.pallas_call(
        _norm_kernel,
        grid=(rows // tile,),
        in_specs=[row(depth), row(depth), _whole((1, depth)), *(row(d.shape[1]) for d in das)],
        out_specs=[row(depth), pl.BlockSpec((1, depth), lambda i: (0, 0))],
        out_shape=[_like((rows, depth)), _like((1, depth), jnp.float32)],
        compiler_params=_params(),
        cost_estimate=_cost(20 * rows * depth, [x, dy, x, x]),
        name="norm_bwd",
    )(x, dy, gain.reshape(1, depth), *das)


def _share_kernel(n, mine_ref, o_ref, held, send_sem, recv_sem):
    me = lax.axis_index("tp")
    barrier = pltpu.get_barrier_semaphore()
    for d in range(1, n):
        pl.semaphore_signal(barrier, inc=1, device_id={"tp": lax.rem(me + d, n)}, device_id_type=pl.DeviceIdType.MESH)
    pl.semaphore_wait(barrier, n - 1)
    copies = []
    for d in range(1, n):
        copy = pltpu.make_async_remote_copy(src_ref=mine_ref, dst_ref=held.at[d - 1], send_sem=send_sem.at[d - 1], recv_sem=recv_sem.at[d - 1],
                                            device_id={"tp": lax.rem(me + d, n)}, device_id_type=pl.DeviceIdType.MESH)
        copy.start()
        copies.append(copy)
    for copy in copies:
        copy.wait()
    total = jnp.zeros(o_ref.shape, jnp.float32)
    for i in range(n):
        other = held[jnp.maximum(lax.rem(me - i + n, n) - 1, 0)]
        total += jnp.where(me == i, mine_ref[...], other)
    o_ref[...] = total


def share_sum(part, n):
    depth = part.shape[1]
    wide = part.reshape(8, depth // 8)
    return pl.pallas_call(
        functools.partial(_share_kernel, n),
        in_specs=[pl.BlockSpec(memory_space=pltpu.VMEM)],
        out_specs=pl.BlockSpec(memory_space=pltpu.VMEM),
        out_shape=_like(wide.shape, jnp.float32),
        scratch_shapes=[pltpu.VMEM((n - 1, *wide.shape), jnp.float32), pltpu.SemaphoreType.DMA((n - 1,)), pltpu.SemaphoreType.DMA((n - 1,))],
        compiler_params=pltpu.CompilerParams(collective_id=0, has_side_effects=True),
        cost_estimate=pl.CostEstimate(flops=n * depth, transcendentals=0, bytes_accessed=8 * depth),
        name="share_sum",
    )(wide).reshape(1, depth)


def solution(mesh):
    n = mesh.shape["tp"]
    cores = 2
    right = [(i, (i + cores) % n) for i in range(n)]
    left = [(i, (i - cores) % n) for i in range(n)]
    other = [(i, i ^ 1) for i in range(n)]

    def program(x, dy, gain, wq, wk, wv, wo):
        block, depth = x.shape
        rows = n * block
        span = block // PARTS
        chips = n // cores
        me = lax.axis_index("tp")
        core, chip = lax.rem(me, cores), lax.div(me, cores)

        def gather(t):
            return lax.all_gather(t, "tp", axis=0, tiled=True)

        def swap(t):
            return lax.ppermute(t, "tp", other)

        half = HEAD // 2
        angle = jnp.arange(rows, dtype=jnp.float32)[:, None] * THETA ** (-jnp.arange(half, dtype=jnp.float32) / half)
        cos, sin = jnp.cos(angle), jnp.sin(angle)
        cos, sin = jnp.concatenate([cos, cos], 1), jnp.concatenate([-sin, sin], 1)

        a = gather(normed(x, gain))
        dys = [gather(dy[s * span : (s + 1) * span]) for s in range(PARTS)]
        w = jnp.concatenate([wq, wk, wv], axis=1)
        pw = swap(w)
        q, k, v = qkv(a, w, cos, sin)
        q = q.reshape(n, PARTS, span, -1)
        seen = [attend(q, k, v, span, block, s * span) for s in range(PARTS)]
        dqs, pqs, carry = [], [], None
        for s in range(PARTS):
            d_out = back_through_wo(dys[s], wo)
            dq, *carry = attend_bwd(q, k, v, d_out, *seen[s], cos, sin, carry, s == PARTS - 1, span, block, s * span)
            dqs.append(dq)
            pqs.append(swap(lax.dynamic_index_in_dim(dq, 1 - core, 0, False)))
        dkv = carry[0]
        dkvs = dkv.reshape(chips, cores, block, 2 * HEAD)
        pkv = swap(lax.dynamic_index_in_dim(dkvs, 1 - core, 1, False))

        width = depth // (2 * PIECES)
        shifts = jnp.array([chips - way * (hop + 1) for hop in range(chips) for way in (1, -1)], jnp.int32)
        places = jnp.stack([jnp.broadcast_to(core, shifts.shape), lax.rem(chip + shifts, chips)], 1)
        das = [None] * (2 * PIECES)
        for hop in range(chips):
            for c in range(PIECES):
                for way, ring in ((1, right), (-1, left)):
                    m = c if way == 1 else PIECES + c
                    if hop:
                        das[m] = lax.ppermute(das[m], "tp", ring)
                    das[m] = grad_a(places, 2 * hop + (way < 0), dqs, dkvs, pqs, pkv, w, pw, das[m], m * width, width)
        by_wo, outs = None, [o for o, _ in seen]
        for skip, steps in WO_STEPS:
            by_wo = grad_wo(outs, dys, by_wo, skip, steps)
        by_qkv = None
        for skip, steps in QKV_STEPS:
            by_qkv = grad_qkv(a, dqs, dkv, by_qkv, skip, steps)
        by_x, by_gain = norm_bwd(x, dy, gain, das)
        return by_x, share_sum(by_gain, n), *by_qkv, by_wo

    tokens, columns = P(("dp", "tp"), None), P(None, "tp")
    return jax.shard_map(
        program,
        mesh=mesh,
        in_specs=(tokens, tokens, P(None), columns, columns, columns, P("tp", None)),
        out_specs=(tokens, P("dp", None), P("dp", "tp"), P("dp", "tp"), P("dp", "tp"), P(("dp", "tp"), None)),
        check_vma=False,
    )
```

```python
import functools

import jax
import jax.numpy as jnp
from jax import lax
from jax.experimental import pallas as pl
from jax.experimental.pallas import tpu as pltpu
from jax.sharding import PartitionSpec as P


NEG = -1e30
HIDDEN = 2 * NEG
LOG2E = 1.4426950408889634
VMEM = 62 * 2**20
HEAD = 128
THETA = 10000
PARTS = 2
DEVS = 2
BK = 512
COLS = 2


def _dot(a, b, ca, cb):
    return lax.dot_general(a, b, (((ca,), (cb,)), ((), ())), preferred_element_type=jnp.float32)


def _whole(shape):
    return pl.BlockSpec(shape, lambda *_: (0,) * len(shape), pipeline_mode=pl.Buffered(1))


def _params(n=1):
    return pltpu.CompilerParams(dimension_semantics=("arbitrary",) * n, vmem_limit_bytes=VMEM)


def _cost(flops, arrays, exps=0):
    return pl.CostEstimate(flops=int(flops), transcendentals=int(exps), bytes_accessed=sum(a.size * a.dtype.itemsize for a in arrays))


def _like(shape, dtype=jnp.bfloat16):
    return jax.ShapeDtypeStruct(shape, dtype)


def _normed_kernel(x_ref, gain_ref, o_ref):
    wide = x_ref[...].astype(jnp.float32)
    scale = lax.rsqrt(jnp.mean(wide * wide, -1, keepdims=True) + 1e-6)
    o_ref[...] = (wide * scale * gain_ref[...].astype(jnp.float32)).astype(jnp.bfloat16)


def normed(x, gain, tile=64):
    rows, depth = x.shape
    row = pl.BlockSpec((tile, depth), lambda i: (i, 0))
    return pl.pallas_call(
        _normed_kernel,
        grid=(rows // tile,),
        in_specs=[row, _whole((1, depth))],
        out_specs=row,
        out_shape=_like((rows, depth)),
        compiler_params=_params(),
        cost_estimate=_cost(6 * rows * depth, [x, x]),
        name="normed",
    )(x, gain.reshape(1, depth))


def _turn(t, cos, sin):
    t = t.astype(jnp.bfloat16).astype(jnp.float32)
    return (t * cos + pltpu.roll(t, HEAD // 2, 1) * sin).astype(jnp.bfloat16)


def _qkv_kernel(a_ref, w_ref, cos_ref, sin_ref, q_ref, k_ref, v_ref):
    cos, sin = cos_ref[...], sin_ref[...]
    wide = q_ref.shape[1]
    got = _dot(a_ref[...], w_ref[...], 1, 0)
    for h in range(0, wide, HEAD):
        q_ref[:, h : h + HEAD] = _turn(got[:, h : h + HEAD], cos, sin)
    k_ref[...] = _turn(got[:, wide : wide + HEAD], cos, sin)
    v_ref[...] = got[:, wide + HEAD :].astype(jnp.bfloat16)


def qkv(a, w, cos, sin, tile=256):
    rows, depth = a.shape
    total = w.shape[1]
    wide = total - 2 * HEAD
    row = lambda n: pl.BlockSpec((tile, n), lambda i: (i, 0))
    return pl.pallas_call(
        _qkv_kernel,
        grid=(rows // tile,),
        in_specs=[row(depth), _whole(w.shape), row(HEAD), row(HEAD)],
        out_specs=[row(wide), row(HEAD), row(HEAD)],
        out_shape=[_like((rows, wide)), _like((rows, HEAD)), _like((rows, HEAD))],
        compiler_params=_params(),
        cost_estimate=_cost(2 * rows * depth * total, [a, w]),
        name="qkv",
    )(a, w, cos, sin)


def _wo_kernel(a_ref, w_ref, o_ref):
    o_ref[...] = _dot(a_ref[...], w_ref[...], 1, 1).astype(jnp.bfloat16)


def back_through_wo(dy, wo, tile=256):
    rows, depth = dy.shape
    return pl.pallas_call(
        _wo_kernel,
        grid=(rows // tile,),
        in_specs=[pl.BlockSpec((tile, depth), lambda i: (i, 0)), _whole(wo.shape)],
        out_specs=pl.BlockSpec((tile, wo.shape[0]), lambda i: (i, 0)),
        out_shape=_like((rows, wo.shape[0])),
        compiler_params=_params(),
        cost_estimate=_cost(2 * rows * depth * wo.shape[0], [dy, wo]),
        name="back_through_wo",
    )(dy, wo)


def _gaps(bk, span, block, start):
    column = lax.broadcasted_iota(jnp.int32, (bk, DEVS * span), 1)
    place = (column // span) * block + start + column % span
    return place - lax.broadcasted_iota(jnp.int32, (bk, DEVS * span), 0)


def _edge(span, block, start):
    return -(-((DEVS - 1) * block + start + span) // 128) * 128


def _forward(q_ref, k_ref, v_ref, o_ref, lse_ref, top_s, mix_s, gap_s, *, span, block, start):
    p = pl.program_id(0)
    heads = q_ref.shape[-1] // HEAD
    scale = HEAD**-0.5
    e = scale * LOG2E
    edge = _edge(span, block, start)
    head = lambda ref, h: ref[:, 0, :, h * HEAD : (h + 1) * HEAD].reshape(-1, HEAD)

    @pl.when(p == 0)
    def _():
        gap_s[...] = _gaps(edge, span, block, start)

    top_s[...] = jnp.full(top_s.shape, NEG, jnp.float32)
    mix_s[...] = jnp.zeros(mix_s.shape, jnp.float32)

    def step(first, n, masked):
        here = pl.ds(first, n)
        k = k_ref[here, :]
        values = jnp.concatenate([v_ref[here, :].T, jnp.ones((8, n), jnp.bfloat16)], axis=0)
        scores = [_dot(k, head(q_ref, h), 1, 1) for h in range(heads)]
        weights, keeps = [], []
        for h, s in enumerate(scores):
            if masked:
                s = jnp.where(gap_s[...] >= 0, s, HIDDEN)
            old = top_s[h : h + 1, :]
            top = jnp.maximum(old, s.max(axis=0, keepdims=True))
            top_s[h : h + 1, :] = top
            weights.append(jnp.exp2((s - top) * e).astype(jnp.bfloat16))
            keeps.append(jnp.exp2((old - top) * e))
        for h in range(heads):
            mix_s[h] = mix_s[h] * keeps[h] + _dot(values, weights[h], 1, 0)

    lax.fori_loop(0, p, lambda j, _: step(j * BK, BK, False), None)
    step(p * BK, edge, True)
    for h in range(heads):
        total = mix_s[h, HEAD : HEAD + 1, :]
        o_ref[:, h * HEAD : (h + 1) * HEAD] = (mix_s[h, :HEAD, :] * (1 / total)).T.astype(jnp.bfloat16)
        lse_ref[h : h + 1, :] = top_s[h : h + 1, :] * scale + jnp.log(total)


def attend(q, k, v, span, block, start):
    devices, _, _, wide = q.shape
    rows = devices * span
    heads = wide // HEAD
    nq = DEVS * span
    edge = _edge(span, block, start)
    row = pl.BlockSpec((nq, wide), lambda i: (i, 0))
    part = pl.BlockSpec((DEVS, 1, span, wide), lambda i: (i, start // span, 0, 0))
    return pl.pallas_call(
        functools.partial(_forward, span=span, block=block, start=start),
        grid=(rows // nq,),
        in_specs=[part, _whole(k.shape), _whole(v.shape)],
        out_specs=[row, pl.BlockSpec((heads, nq), lambda i: (0, i))],
        out_shape=[_like((rows, wide)), _like((heads, rows), jnp.float32)],
        scratch_shapes=[pltpu.VMEM((heads, nq), jnp.float32), pltpu.VMEM((heads, HEAD + 8, nq), jnp.float32), pltpu.VMEM((edge, nq), jnp.int32)],
        compiler_params=_params(),
        cost_estimate=_cost(2 * rows * wide * k.shape[0] * 2, [q, k, v], rows * heads * k.shape[0]),
        name="attend",
    )(q, k, v)


def _backward(*refs, span, block, start, carried, last):
    q_ref, k_ref, v_ref, do_ref, o_ref, lse_ref, cos_ref, sin_ref, *refs = refs
    if carried:
        dk_in, dv_in, *refs = refs
    if last:
        kcos_ref, ksin_ref, dq_ref, dkv_ref, *refs = refs
    else:
        dq_ref, dk_ref, dv_ref, *refs = refs
    dq_s, dk_s, dv_s, gap_s = refs
    p = pl.program_id(0)
    heads = q_ref.shape[-1] // HEAD
    scale = HEAD**-0.5
    e = scale * LOG2E
    edge = _edge(span, block, start)

    @pl.when(p == 0)
    def _():
        gap_s[...] = _gaps(edge, span, block, start)
        dk_s[...] = dk_in[...] if carried else jnp.zeros(dk_s.shape, jnp.float32)
        dv_s[...] = dv_in[...] if carried else jnp.zeros(dv_s.shape, jnp.float32)

    dq_s[...] = jnp.zeros(dq_s.shape, jnp.float32)
    part = lambda ref, h: ref[:, 0, :, h * HEAD : (h + 1) * HEAD].reshape(-1, HEAD)
    head = lambda ref, h: ref[:, h * HEAD : (h + 1) * HEAD]
    lses = [lse_ref[h : h + 1, :] * LOG2E for h in range(heads)]
    deltas = [(head(do_ref, h).astype(jnp.float32) * head(o_ref, h).astype(jnp.float32)).T.sum(axis=0, keepdims=True) for h in range(heads)]

    def step(first, n, masked):
        here = pl.ds(first, n)
        k, v = k_ref[here, :], v_ref[here, :]
        kt = k.T
        scores = [_dot(k, part(q_ref, h), 1, 1) for h in range(heads)]
        dps = [_dot(v, head(do_ref, h), 1, 1) for h in range(heads)]
        for h in range(heads):
            w = jnp.exp2(scores[h] * e - lses[h])
            if masked:
                w = jnp.where(gap_s[...] >= 0, w, 0.0)
            ds = (w * (dps[h] - deltas[h])).astype(jnp.bfloat16)
            dv_s[here, :] += _dot(w.astype(jnp.bfloat16), head(do_ref, h), 1, 0)
            dk_s[here, :] += _dot(ds, part(q_ref, h), 1, 0)
            dq_s[h] += _dot(kt, ds, 1, 0)

    lax.fori_loop(0, p, lambda j, _: step(j * BK, BK, False), None)
    step(p * BK, edge, True)
    cos, sin = (r[:, 0].reshape(-1, HEAD) for r in (cos_ref, sin_ref))
    for h in range(heads):
        dq_ref[:, 0, :, h * HEAD : (h + 1) * HEAD] = _turn((dq_s[h] * scale).T, cos, -sin).reshape(DEVS, span, HEAD)

    @pl.when(p == pl.num_programs(0) - 1)
    def _():
        if last:
            dkv_ref[:, :HEAD] = _turn(dk_s[...] * scale, kcos_ref[...], -ksin_ref[...])
            dkv_ref[:, HEAD:] = dv_s[...].astype(jnp.bfloat16)
        else:
            dk_ref[...] = dk_s[...]
            dv_ref[...] = dv_s[...]


def attend_bwd(q, k, v, d_out, out, lse, cos, sin, carry, last, span, block, start):
    devices, _, _, wide = q.shape
    rows = devices * span
    heads = wide // HEAD
    nq = DEVS * span
    keys = k.shape[0]
    edge = _edge(span, block, start)
    row = pl.BlockSpec((nq, wide), lambda i: (i, 0))
    part = lambda w: pl.BlockSpec((DEVS, 1, span, w), lambda i: (i, start // span, 0, 0))
    kv = _whole(k.shape)
    more = [*(carry or ()), *((cos, sin) if last else ())]
    tables = [t.reshape(devices, -1, span, HEAD) for t in (cos, sin)]
    sums = [(keys, 2 * HEAD)] if last else [k.shape, k.shape]
    return pl.pallas_call(
        functools.partial(_backward, span=span, block=block, start=start, carried=carry is not None, last=last),
        grid=(rows // nq,),
        in_specs=[part(wide), kv, kv, row, row, pl.BlockSpec((heads, nq), lambda i: (0, i)), part(HEAD), part(HEAD)] + [kv] * len(more),
        out_specs=[pl.BlockSpec((DEVS, 1, span, wide), lambda i: (0, i, 0, 0)), *(_whole(t) for t in sums)],
        out_shape=[_like((DEVS, devices // DEVS, span, wide)), *(_like(t, jnp.bfloat16 if last else jnp.float32) for t in sums)],
        scratch_shapes=[pltpu.VMEM((heads, HEAD, nq), jnp.float32), pltpu.VMEM((keys, HEAD), jnp.float32),
                        pltpu.VMEM((keys, HEAD), jnp.float32), pltpu.VMEM((edge, nq), jnp.int32)],
        compiler_params=_params(),
        cost_estimate=_cost(2 * rows * wide * keys * 5, [d_out, out, k, v, k, v], rows * heads * keys),
        name="attend_bwd",
    )(q, k, v, d_out, out, lse, *tables, *more)


def _da_kernel(core_ref, *refs, parts):
    dqs, (dkv_ref, *refs) = refs[:parts], refs[parts:]
    pqs, (pkv_ref, w_ref, pw_ref, o_ref, mine_s, other_s) = refs[:parts], refs[parts:]
    chips, span, wide = pqs[0].shape
    block = parts * span

    @pl.when(pl.program_id(0) == 0)
    def _():
        for j in range(chips):
            for n in range(parts):
                at = j * block + n * span
                mine_s[at : at + span, :wide] = dqs[n][0, j]
                other_s[at : at + span, :wide] = pqs[n][j]
            mine_s[j * block : (j + 1) * block, wide:] = dkv_ref[j, 0]
            other_s[j * block : (j + 1) * block, wide:] = pkv_ref[j]

    o_ref[...] = (_dot(mine_s[...], w_ref[...], 1, 1) + _dot(other_s[...], pw_ref[...], 1, 1)).astype(jnp.bfloat16)


def grad_a(core, dqs, dkv, pqs, pkv, w, pw, first, columns, tile=512):
    chips, span, wide = pqs[0].shape
    block = len(dqs) * span
    rows, depth = chips * block, w.shape[1]
    skip = first // tile
    once = dict(pipeline_mode=pl.Buffered(1))
    weights = pl.BlockSpec((tile, depth), lambda i, core: (i + skip, 0))
    return pl.pallas_call(
        functools.partial(_da_kernel, parts=len(dqs)),
        grid_spec=pltpu.PrefetchScalarGridSpec(
            num_scalar_prefetch=1,
            grid=(columns // tile,),
            in_specs=[*(pl.BlockSpec((1, chips, span, wide), lambda i, core: (core[0], 0, 0, 0), **once) for _ in dqs),
                      pl.BlockSpec((chips, 1, block, 2 * HEAD), lambda i, core: (0, core[0], 0, 0), **once),
                      *(_whole(t.shape) for t in pqs), _whole(pkv.shape), weights, weights],
            out_specs=pl.BlockSpec((rows, tile), lambda i, core: (0, i)),
            scratch_shapes=[pltpu.VMEM((rows, depth), jnp.bfloat16), pltpu.VMEM((rows, depth), jnp.bfloat16)],
        ),
        out_shape=_like((rows, columns)),
        compiler_params=_params(),
        cost_estimate=pl.CostEstimate(flops=4 * rows * columns * depth, transcendentals=0, bytes_accessed=4 * columns * depth),
        name="grad_a",
    )(core, *dqs, dkv, *pqs, pkv, w, pw)


def _dw_kernel(*refs, parts, span):
    x_ref, *refs = refs
    dqs, refs = refs[:parts], refs[parts:]
    dkv_ref, *refs = refs
    oq_ref, ok_ref, ov_ref, cat_s = refs[-4:]
    wide = oq_ref.shape[1]

    @pl.when(pl.program_id(0) == 0)
    def _():
        cat_s[:, wide:] = dkv_ref[...]
        cores, chips = dqs[0].shape[:2]
        for chip in range(chips):
            for core in range(cores):
                for n in range(parts):
                    at = ((chip * cores + core) * parts + n) * span
                    cat_s[at : at + span, :wide] = dqs[n][core, chip]

    got = _dot(x_ref[...], cat_s[...], 0, 0)
    oq_ref[...] = got[:, :wide].astype(jnp.bfloat16)
    ok_ref[...] = got[:, wide : wide + HEAD].astype(jnp.bfloat16)
    ov_ref[...] = got[:, wide + HEAD :].astype(jnp.bfloat16)


def grad_qkv(x, dqs, dkv, tile=512):
    rows, depth = x.shape
    wide = dqs[0].shape[-1]
    shapes = [(depth, wide), (depth, HEAD), (depth, HEAD)]
    given = [x, *dqs, dkv]
    return pl.pallas_call(
        functools.partial(_dw_kernel, parts=len(dqs), span=dqs[0].shape[-2]),
        grid=(depth // tile,),
        in_specs=[pl.BlockSpec((rows, tile), lambda i: (0, i)), *(_whole(t.shape) for t in given[1:])],
        out_specs=[pl.BlockSpec((tile, t[1]), lambda i: (i, 0)) for t in shapes],
        out_shape=[_like(t) for t in shapes],
        scratch_shapes=[pltpu.VMEM((rows, wide + 2 * HEAD), jnp.bfloat16)],
        compiler_params=_params(),
        cost_estimate=_cost(2 * rows * depth * (wide + 2 * HEAD), given),
        name="grad_qkv",
    )(*given)


def _dwo_kernel(*refs, parts):
    outs, dys, o_ref = refs[:parts], refs[parts : 2 * parts], refs[-1]
    got = _dot(outs[0][...], dys[0][...], 0, 0)
    for n in range(1, parts):
        got += _dot(outs[n][...], dys[n][...], 0, 0)
    o_ref[...] = got.astype(jnp.bfloat16)


def grad_wo(outs, dys, tile=512):
    rows, depth = dys[0].shape
    wide = outs[0].shape[1]
    given = [*outs, *dys]
    return pl.pallas_call(
        functools.partial(_dwo_kernel, parts=len(outs)),
        grid=(depth // tile,),
        in_specs=[*(_whole(x.shape) for x in outs), *(pl.BlockSpec((rows, tile), lambda i: (0, i)) for _ in dys)],
        out_specs=pl.BlockSpec((wide, tile), lambda i: (0, i)),
        out_shape=_like((wide, depth)),
        compiler_params=_params(),
        cost_estimate=_cost(2 * len(outs) * rows * depth * wide, given),
        name="grad_wo",
    )(*given)


def _norm_kernel(*refs):
    x_ref, dy_ref, gain_ref, *das, o_ref, og_ref = refs
    x = x_ref[...].astype(jnp.float32)
    scale = lax.rsqrt(jnp.mean(x * x, -1, keepdims=True) + 1e-6)
    da = jnp.concatenate([r[...].astype(jnp.float32) for r in das], axis=1)
    unit = x * scale
    by_unit = da * gain_ref[...].astype(jnp.float32)
    mean = jnp.mean(by_unit * unit, -1, keepdims=True)
    o_ref[...] = (dy_ref[...].astype(jnp.float32) + scale * (by_unit - unit * mean)).astype(jnp.bfloat16)
    part = jnp.sum(da * unit, axis=0, keepdims=True)

    @pl.when(pl.program_id(0) == 0)
    def _():
        og_ref[...] = part

    @pl.when(pl.program_id(0) > 0)
    def _():
        og_ref[...] += part


def norm_bwd(x, dy, gain, das, tile=32):
    rows, depth = x.shape
    row = lambda n: pl.BlockSpec((tile, n), lambda i: (i, 0))
    return pl.pallas_call(
        _norm_kernel,
        grid=(rows // tile,),
        in_specs=[row(depth), row(depth), _whole((1, depth)), *(row(d.shape[1]) for d in das)],
        out_specs=[row(depth), pl.BlockSpec((1, depth), lambda i: (0, 0))],
        out_shape=[_like((rows, depth)), _like((1, depth), jnp.float32)],
        compiler_params=_params(),
        cost_estimate=_cost(20 * rows * depth, [x, dy, x, x]),
        name="norm_bwd",
    )(x, dy, gain.reshape(1, depth), *das)


def _share_kernel(n, mine_ref, o_ref, held, send_sem, recv_sem):
    me = lax.axis_index("tp")
    barrier = pltpu.get_barrier_semaphore()
    for d in range(1, n):
        pl.semaphore_signal(barrier, inc=1, device_id={"tp": lax.rem(me + d, n)}, device_id_type=pl.DeviceIdType.MESH)
    pl.semaphore_wait(barrier, n - 1)
    copies = []
    for d in range(1, n):
        copy = pltpu.make_async_remote_copy(src_ref=mine_ref, dst_ref=held.at[d - 1], send_sem=send_sem.at[d - 1], recv_sem=recv_sem.at[d - 1],
                                            device_id={"tp": lax.rem(me + d, n)}, device_id_type=pl.DeviceIdType.MESH)
        copy.start()
        copies.append(copy)
    for copy in copies:
        copy.wait()
    total = jnp.zeros(o_ref.shape, jnp.float32)
    for i in range(n):
        other = held[jnp.maximum(lax.rem(me - i + n, n) - 1, 0)]
        total += jnp.where(me == i, mine_ref[...], other)
    o_ref[...] = total


def share_sum(part, n):
    depth = part.shape[1]
    wide = part.reshape(8, depth // 8)
    return pl.pallas_call(
        functools.partial(_share_kernel, n),
        in_specs=[pl.BlockSpec(memory_space=pltpu.VMEM)],
        out_specs=pl.BlockSpec(memory_space=pltpu.VMEM),
        out_shape=_like(wide.shape, jnp.float32),
        scratch_shapes=[pltpu.VMEM((n - 1, *wide.shape), jnp.float32), pltpu.SemaphoreType.DMA((n - 1,)), pltpu.SemaphoreType.DMA((n - 1,))],
        compiler_params=pltpu.CompilerParams(collective_id=0, has_side_effects=True),
        cost_estimate=pl.CostEstimate(flops=n * depth, transcendentals=0, bytes_accessed=8 * depth),
        name="share_sum",
    )(wide).reshape(1, depth)


def solution(mesh):
    n = mesh.shape["tp"]
    cores = 2
    same = [list(range(c, n, cores)) for c in range(cores)]
    other = [(i, i ^ 1) for i in range(n)]

    def program(x, dy, gain, wq, wk, wv, wo):
        block, depth = x.shape
        rows = n * block
        span = block // PARTS
        chips = n // cores
        me = lax.axis_index("tp")
        core = lax.rem(me, cores)

        def gather(t):
            return lax.all_gather(t, "tp", axis=0, tiled=True)

        def swap(t):
            return lax.ppermute(t, "tp", other)

        half = HEAD // 2
        angle = jnp.arange(rows, dtype=jnp.float32)[:, None] * THETA ** (-jnp.arange(half, dtype=jnp.float32) / half)
        cos, sin = jnp.cos(angle), jnp.sin(angle)
        cos, sin = jnp.concatenate([cos, cos], 1), jnp.concatenate([-sin, sin], 1)

        a = gather(normed(x, gain))
        dys = [gather(dy[s * span : (s + 1) * span]) for s in range(PARTS)]
        w = jnp.concatenate([wq, wk, wv], axis=1)
        pw = swap(w)
        q, k, v = qkv(a, w, cos, sin)
        q = q.reshape(n, PARTS, span, -1)
        seen = [attend(q, k, v, span, block, s * span) for s in range(PARTS)]
        dqs, pqs, carry = [], [], None
        for s in range(PARTS):
            d_out = back_through_wo(dys[s], wo)
            dq, *carry = attend_bwd(q, k, v, d_out, *seen[s], cos, sin, carry, s == PARTS - 1, span, block, s * span)
            dqs.append(dq)
            pqs.append(swap(lax.dynamic_index_in_dim(dq, 1 - core, 0, False)))
        dkv = carry[0]
        dkvs = dkv.reshape(chips, cores, block, 2 * HEAD)
        pkv = swap(lax.dynamic_index_in_dim(dkvs, 1 - core, 1, False))

        width = depth // COLS
        das = []
        for c in range(COLS):
            term = grad_a(core[None], dqs, dkvs, pqs, pkv, w, pw, c * width, width)
            das.append(lax.psum_scatter(term, "tp", scatter_dimension=0, axis_index_groups=same, tiled=True))
        by_wo = grad_wo([o for o, _ in seen], dys)
        by_qkv = grad_qkv(a, dqs, dkv)
        by_x, by_gain = norm_bwd(x, dy, gain, das)
        return by_x, share_sum(by_gain, n), *by_qkv, by_wo

    tokens, columns = P(("dp", "tp"), None), P(None, "tp")
    return jax.shard_map(
        program,
        mesh=mesh,
        in_specs=(tokens, tokens, P(None), columns, columns, columns, P("tp", None)),
        out_specs=(tokens, P("dp", None), P("dp", "tp"), P("dp", "tp"), P("dp", "tp"), P(("dp", "tp"), None)),
        check_vma=False,
    )
```

```python
import functools

import jax
import jax.numpy as jnp
from jax import lax
from jax.experimental import pallas as pl
from jax.experimental.pallas import tpu as pltpu
from jax.sharding import PartitionSpec as P


NEG = -1e30
HIDDEN = 2 * NEG
LOG2E = 1.4426950408889634
VMEM = 62 * 2**20
HEAD = 128
THETA = 10000
PARTS = 2
DEVS = 2
BK = 512
COLS = 2


def _dot(a, b, ca, cb):
    return lax.dot_general(a, b, (((ca,), (cb,)), ((), ())), preferred_element_type=jnp.float32)


def _whole(shape):
    return pl.BlockSpec(shape, lambda *_: (0,) * len(shape), pipeline_mode=pl.Buffered(1))


def _params(n=1):
    return pltpu.CompilerParams(dimension_semantics=("arbitrary",) * n, vmem_limit_bytes=VMEM)


def _cost(flops, arrays, exps=0):
    return pl.CostEstimate(flops=int(flops), transcendentals=int(exps), bytes_accessed=sum(a.size * a.dtype.itemsize for a in arrays))


def _like(shape, dtype=jnp.bfloat16):
    return jax.ShapeDtypeStruct(shape, dtype)


def _normed_kernel(x_ref, gain_ref, o_ref):
    wide = x_ref[...].astype(jnp.float32)
    scale = lax.rsqrt(jnp.mean(wide * wide, -1, keepdims=True) + 1e-6)
    o_ref[...] = (wide * scale * gain_ref[...].astype(jnp.float32)).astype(jnp.bfloat16)


def normed(x, gain, tile=64):
    rows, depth = x.shape
    row = pl.BlockSpec((tile, depth), lambda i: (i, 0))
    return pl.pallas_call(
        _normed_kernel,
        grid=(rows // tile,),
        in_specs=[row, _whole((1, depth))],
        out_specs=row,
        out_shape=_like((rows, depth)),
        compiler_params=_params(),
        cost_estimate=_cost(6 * rows * depth, [x, x]),
        name="normed",
    )(x, gain.reshape(1, depth))


def _turn(t, cos, sin):
    t = t.astype(jnp.bfloat16).astype(jnp.float32)
    return (t * cos + pltpu.roll(t, HEAD // 2, 1) * sin).astype(jnp.bfloat16)


def _fetch(at_ref, pieces, rows_s, sem, columns=None):
    copies = []
    for n, piece in enumerate(pieces):
        rows = piece.shape[0]
        place = rows_s.at[pl.ds(pl.multiple_of(at_ref[n], rows), rows)]
        copies.append(pltpu.make_async_copy(piece if columns is None else piece.at[:, columns], place, sem))
    return copies


def _all_here(at_ref, pieces, rows_s, sem):
    @pl.when(pl.program_id(0) == 0)
    def _():
        copies = _fetch(at_ref, pieces, rows_s, sem)
        for copy in copies:
            copy.start()
        for copy in copies:
            copy.wait()


def _qkv_kernel(table_ref, at_ref, *refs, pieces, carried):
    given, (w_ref, cos_ref, sin_ref, *refs) = refs[:pieces], refs[pieces:]
    q_ref, k_ref, v_ref, rows_s, sem = refs[carried:]
    _all_here(at_ref, given, rows_s, sem)
    i = pl.program_id(0)
    wide = q_ref.shape[-1]
    rows = DEVS * q_ref.shape[2]
    flat = lambda ref: ref[:, 0].reshape(rows, HEAD)
    fold = lambda t: t.reshape(DEVS, -1, t.shape[-1])
    cos, sin = flat(cos_ref), flat(sin_ref)
    got = _dot(rows_s[pl.ds(pl.multiple_of(i * rows, rows), rows), :], w_ref[...], 1, 0)
    for h in range(0, wide, HEAD):
        q_ref[:, 0, :, h : h + HEAD] = fold(_turn(got[:, h : h + HEAD], cos, sin))
    k_ref[:, 0] = fold(_turn(got[:, wide : wide + HEAD], cos, sin))
    v_ref[:, 0] = fold(got[:, wide + HEAD :].astype(jnp.bfloat16))


def _step_spec(span, wide):
    return pl.BlockSpec((DEVS, 1, span, wide), lambda i, table, *_: (table[i, 0], table[i, 1], 0, 0))


def qkv(table, at, pieces, w, cos, sin, sofar):
    devices, parts, span, _ = cos.shape
    depth, total = w.shape
    wide = total - 2 * HEAD
    steps = table.shape[0]
    rows = steps * DEVS * span
    sofar = sofar or ()
    any_ = pl.BlockSpec(memory_space=pl.ANY)
    widths = (wide, HEAD, HEAD)
    return pl.pallas_call(
        functools.partial(_qkv_kernel, pieces=len(pieces), carried=len(sofar)),
        grid_spec=pltpu.PrefetchScalarGridSpec(
            num_scalar_prefetch=2,
            grid=(steps,),
            in_specs=[*(any_ for _ in pieces), _whole(w.shape), _step_spec(span, HEAD), _step_spec(span, HEAD), *(any_ for _ in sofar)],
            out_specs=[_step_spec(span, n) for n in widths],
            scratch_shapes=[pltpu.VMEM((rows, depth), jnp.bfloat16), pltpu.SemaphoreType.DMA],
        ),
        out_shape=[_like((devices, parts, span, n)) for n in widths],
        input_output_aliases={2 + len(pieces) + 3 + n: n for n in range(len(sofar))},
        compiler_params=_params(),
        cost_estimate=pl.CostEstimate(flops=2 * rows * depth * total, transcendentals=0, bytes_accessed=2 * depth * (rows + total)),
        name="qkv",
    )(table, at, *pieces, w, cos, sin, *sofar)


def _wo_kernel(at_ref, *refs, pieces):
    given, (w_ref, o_ref, rows_s, sem) = refs[:pieces], refs[pieces:]
    _all_here(at_ref, given, rows_s, sem)
    rows = o_ref.shape[0]
    here = pl.ds(pl.multiple_of(pl.program_id(0) * rows, rows), rows)
    o_ref[...] = _dot(rows_s[here, :], w_ref[...], 1, 1).astype(jnp.bfloat16)


def back_through_wo(at, pieces, wo, tile=256):
    rows, depth = sum(p.shape[0] for p in pieces), wo.shape[1]
    return pl.pallas_call(
        functools.partial(_wo_kernel, pieces=len(pieces)),
        grid_spec=pltpu.PrefetchScalarGridSpec(
            num_scalar_prefetch=1,
            grid=(rows // tile,),
            in_specs=[*(pl.BlockSpec(memory_space=pl.ANY) for _ in pieces), _whole(wo.shape)],
            out_specs=pl.BlockSpec((tile, wo.shape[0]), lambda i, at: (i, 0)),
            scratch_shapes=[pltpu.VMEM((rows, depth), jnp.bfloat16), pltpu.SemaphoreType.DMA],
        ),
        out_shape=_like((rows, wo.shape[0])),
        compiler_params=_params(),
        cost_estimate=pl.CostEstimate(flops=2 * rows * depth * wo.shape[0], transcendentals=0, bytes_accessed=2 * depth * (rows + wo.shape[0])),
        name="back_through_wo",
    )(at, *pieces, wo)


def _gaps(span):
    column = lax.broadcasted_iota(jnp.int32, (BK, DEVS * span), 1)
    place = (column // span) * (span * PARTS) + column % span
    return place - lax.broadcasted_iota(jnp.int32, (BK, DEVS * span), 0)


def _part(ref, h):
    return ref[:, 0, :, h * HEAD : (h + 1) * HEAD].reshape(-1, HEAD)


def _forward(q_ref, k_ref, v_ref, o_ref, lse_ref, top_s, mix_s, gap_s):
    chip, half = pl.program_id(0), pl.program_id(1)
    span = q_ref.shape[2]
    heads = q_ref.shape[-1] // HEAD
    scale = HEAD**-0.5
    e = scale * LOG2E

    @pl.when((chip == 0) & (half == 0))
    def _():
        gap_s[...] = _gaps(span)

    top_s[...] = jnp.full(top_s.shape, NEG, jnp.float32)
    mix_s[...] = jnp.zeros(mix_s.shape, jnp.float32)

    def step(j, masked):
        here = pl.ds(pl.multiple_of(j * BK, BK), BK)
        k = k_ref[here, :]
        values = jnp.concatenate([v_ref[here, :].T, jnp.ones((8, BK), jnp.bfloat16)], axis=0)
        scores = [_dot(k, _part(q_ref, h), 1, 1) for h in range(heads)]
        weights, keeps = [], []
        for h, s in enumerate(scores):
            if masked:
                s = jnp.where(gap_s[...] >= -half * span, s, HIDDEN)
            old = top_s[h : h + 1, :]
            top = jnp.maximum(old, s.max(axis=0, keepdims=True))
            top_s[h : h + 1, :] = top
            weights.append(jnp.exp2((s - top) * e).astype(jnp.bfloat16))
            keeps.append(jnp.exp2((old - top) * e))
        for h in range(heads):
            mix_s[h] = mix_s[h] * keeps[h] + _dot(values, weights[h], 1, 0)

    lax.fori_loop(0, chip, lambda j, _: step(j, False), None)
    step(chip, True)
    for h in range(heads):
        total = mix_s[h, HEAD : HEAD + 1, :]
        o_ref[:, 0, :, h * HEAD : (h + 1) * HEAD] = (mix_s[h, :HEAD, :] * (1 / total)).T.astype(jnp.bfloat16).reshape(DEVS, span, HEAD)
        lse_ref[0, 0, h : h + 1, :] = top_s[h : h + 1, :] * scale + jnp.log(total)


def attend(q, k, v):
    devices, parts, span, wide = q.shape
    heads, nq, keys = wide // HEAD, DEVS * span, k.shape[0]
    chips = devices // DEVS
    part = pl.BlockSpec((DEVS, 1, span, wide), lambda i, j: (i, j, 0, 0))
    return pl.pallas_call(
        _forward,
        grid=(chips, parts),
        in_specs=[part, _whole(k.shape), _whole(v.shape)],
        out_specs=[part, pl.BlockSpec((1, 1, heads, nq), lambda i, j: (i, j, 0, 0))],
        out_shape=[_like(q.shape), _like((chips, parts, heads, nq), jnp.float32)],
        scratch_shapes=[pltpu.VMEM((heads, nq), jnp.float32), pltpu.VMEM((heads, HEAD + 8, nq), jnp.float32), pltpu.VMEM((BK, nq), jnp.int32)],
        compiler_params=_params(2),
        cost_estimate=_cost(2 * q.size * keys * 2, [q, k, v, q], q.size // HEAD * keys),
        name="attend",
    )(q, k, v)


def _backward(table_ref, *refs, first, last):
    q_ref, k_ref, v_ref, do_ref, o_ref, lse_ref, cos_ref, sin_ref, *refs = refs
    if not first:
        dk_in, dv_in, _, *refs = refs
    if last:
        kcos_ref, ksin_ref, dq_ref, dkv_ref, *refs = refs
    else:
        dq_ref, dk_ref, dv_ref, *refs = refs
    dq_s, dk_s, dv_s, gap_s = refs
    i = pl.program_id(0)
    chip, half = table_ref[i, 0], table_ref[i, 1]
    span = q_ref.shape[2]
    heads = q_ref.shape[-1] // HEAD
    scale = HEAD**-0.5
    e = scale * LOG2E

    @pl.when(i == 0)
    def _():
        gap_s[...] = _gaps(span)
        dk_s[...] = jnp.zeros(dk_s.shape, jnp.float32) if first else dk_in[...]
        dv_s[...] = jnp.zeros(dv_s.shape, jnp.float32) if first else dv_in[...]

    dq_s[...] = jnp.zeros(dq_s.shape, jnp.float32)
    head = lambda ref, h: ref[:, h * HEAD : (h + 1) * HEAD]
    lses = [lse_ref[0, 0, h : h + 1, :] * LOG2E for h in range(heads)]
    deltas = [(head(do_ref, h).astype(jnp.float32) * _part(o_ref, h).astype(jnp.float32)).T.sum(axis=0, keepdims=True) for h in range(heads)]

    def step(j, masked):
        here = pl.ds(pl.multiple_of(j * BK, BK), BK)
        k, v = k_ref[here, :], v_ref[here, :]
        kt = k.T
        scores = [_dot(k, _part(q_ref, h), 1, 1) for h in range(heads)]
        dps = [_dot(v, head(do_ref, h), 1, 1) for h in range(heads)]
        for h in range(heads):
            w = jnp.exp2(scores[h] * e - lses[h])
            if masked:
                w = jnp.where(gap_s[...] >= -half * span, w, 0.0)
            ds = (w * (dps[h] - deltas[h])).astype(jnp.bfloat16)
            dv_s[here, :] += _dot(w.astype(jnp.bfloat16), head(do_ref, h), 1, 0)
            dk_s[here, :] += _dot(ds, _part(q_ref, h), 1, 0)
            dq_s[h] += _dot(kt, ds, 1, 0)

    lax.fori_loop(0, chip, lambda j, _: step(j, False), None)
    step(chip, True)
    cos, sin = (r[:, 0].reshape(-1, HEAD) for r in (cos_ref, sin_ref))
    for h in range(heads):
        dq_ref[:, 0, 0, :, h * HEAD : (h + 1) * HEAD] = _turn((dq_s[h] * scale).T, cos, -sin).reshape(DEVS, span, HEAD)

    @pl.when(i == pl.num_programs(0) - 1)
    def _():
        if last:
            dkv_ref[:, :HEAD] = _turn(dk_s[...] * scale, kcos_ref[...], -ksin_ref[...])
            dkv_ref[:, HEAD:] = dv_s[...].astype(jnp.bfloat16)
        else:
            dk_ref[...] = dk_s[...]
            dv_ref[...] = dv_s[...]


def attend_bwd(table, q, k, v, d_out, out, lse, cos, sin, sofar, last):
    devices, parts, span, wide = q.shape
    heads, nq, keys = wide // HEAD, DEVS * span, k.shape[0]
    chips = devices // DEVS
    steps = table.shape[0]
    kv = _whole(k.shape)
    dq_shape = (DEVS, chips, parts, span, wide)
    more, specs = [], []
    if sofar is not None:
        dq, dk, dv = sofar
        more, specs = [dk, dv, dq], [kv, kv, pl.BlockSpec(memory_space=pl.ANY)]
    if last:
        more, specs = [*more, cos.reshape(keys, HEAD), sin.reshape(keys, HEAD)], [*specs, kv, kv]
    sums = [(keys, 2 * HEAD)] if last else [k.shape, k.shape]
    return pl.pallas_call(
        functools.partial(_backward, first=sofar is None, last=last),
        grid_spec=pltpu.PrefetchScalarGridSpec(
            num_scalar_prefetch=1,
            grid=(steps,),
            in_specs=[_step_spec(span, wide), kv, kv, pl.BlockSpec((nq, wide), lambda i, table: (i, 0)), _step_spec(span, wide),
                      pl.BlockSpec((1, 1, heads, nq), lambda i, table: (table[i, 0], table[i, 1], 0, 0)),
                      _step_spec(span, HEAD), _step_spec(span, HEAD), *specs],
            out_specs=[pl.BlockSpec((DEVS, 1, 1, span, wide), lambda i, table: (0, table[i, 0], table[i, 1], 0, 0)), *(_whole(t) for t in sums)],
            scratch_shapes=[pltpu.VMEM((heads, HEAD, nq), jnp.float32), pltpu.VMEM((keys, HEAD), jnp.float32),
                            pltpu.VMEM((keys, HEAD), jnp.float32), pltpu.VMEM((BK, nq), jnp.int32)],
        ),
        out_shape=[_like(dq_shape), *(_like(t, jnp.bfloat16 if last else jnp.float32) for t in sums)],
        input_output_aliases={} if sofar is None else {11: 0},
        compiler_params=_params(),
        cost_estimate=pl.CostEstimate(flops=2 * steps * nq * wide * keys * 5, transcendentals=steps * nq * heads * keys, bytes_accessed=8 * steps * nq * wide),
        name="attend_bwd",
    )(table, q, k, v, d_out, out, lse, cos, sin, *more)


def _da_kernel(core_ref, dq_ref, dkv_ref, pq_ref, pkv_ref, w_ref, pw_ref, o_ref, mine_s, other_s):
    chips, parts, span, wide = pq_ref.shape
    block = parts * span

    @pl.when(pl.program_id(0) == 0)
    def _():
        for j in range(chips):
            for n in range(parts):
                at = j * block + n * span
                mine_s[at : at + span, :wide] = dq_ref[0, j, n]
                other_s[at : at + span, :wide] = pq_ref[j, n]
            mine_s[j * block : (j + 1) * block, wide:] = dkv_ref[j, 0]
            other_s[j * block : (j + 1) * block, wide:] = pkv_ref[j]

    o_ref[...] = (_dot(mine_s[...], w_ref[...], 1, 1) + _dot(other_s[...], pw_ref[...], 1, 1)).astype(jnp.bfloat16)


def grad_a(core, dq, dkv, pq, pkv, w, pw, first, columns, tile=512):
    chips, parts, span, wide = pq.shape
    block = parts * span
    rows, depth = chips * block, w.shape[1]
    skip = first // tile
    once = dict(pipeline_mode=pl.Buffered(1))
    weights = pl.BlockSpec((tile, depth), lambda i, core: (i + skip, 0))
    return pl.pallas_call(
        _da_kernel,
        grid_spec=pltpu.PrefetchScalarGridSpec(
            num_scalar_prefetch=1,
            grid=(columns // tile,),
            in_specs=[pl.BlockSpec((1, chips, parts, span, wide), lambda i, core: (core[0], 0, 0, 0, 0), **once),
                      pl.BlockSpec((chips, 1, block, 2 * HEAD), lambda i, core: (0, core[0], 0, 0), **once),
                      _whole(pq.shape), _whole(pkv.shape), weights, weights],
            out_specs=pl.BlockSpec((rows, tile), lambda i, core: (0, i)),
            scratch_shapes=[pltpu.VMEM((rows, depth), jnp.bfloat16), pltpu.VMEM((rows, depth), jnp.bfloat16)],
        ),
        out_shape=_like((rows, columns)),
        compiler_params=_params(),
        cost_estimate=pl.CostEstimate(flops=4 * rows * columns * depth, transcendentals=0, bytes_accessed=4 * columns * depth),
        name="grad_a",
    )(core, dq, dkv, pq, pkv, w, pw)


def _columns_here(at_ref, pieces, rows_s, sem):
    i, steps = pl.program_id(0), pl.num_programs(0)
    tile = rows_s.shape[-1]

    def copies(step):
        slot = lax.rem(step, 2)
        return _fetch(at_ref, pieces, rows_s.at[slot], sem.at[slot], pl.ds(pl.multiple_of(step * tile, tile), tile))

    @pl.when(i == 0)
    def _():
        for copy in copies(i):
            copy.start()

    @pl.when(i + 1 < steps)
    def _():
        for copy in copies(i + 1):
            copy.start()

    for copy in copies(i):
        copy.wait()
    return rows_s[lax.rem(i, 2)]


def _dw_kernel(at_ref, *refs, pieces):
    given, (dq_ref, dkv_ref, oq_ref, ok_ref, ov_ref, cat_s, rows_s, sem) = refs[:pieces], refs[pieces:]
    wide = oq_ref.shape[1]

    @pl.when(pl.program_id(0) == 0)
    def _():
        cat_s[:, wide:] = dkv_ref[...]
        cores, chips, parts, span, _ = dq_ref.shape
        for chip in range(chips):
            for core in range(cores):
                for n in range(parts):
                    at = ((chip * cores + core) * parts + n) * span
                    cat_s[at : at + span, :wide] = dq_ref[core, chip, n]

    got = _dot(_columns_here(at_ref, given, rows_s, sem), cat_s[...], 0, 0)
    oq_ref[...] = got[:, :wide].astype(jnp.bfloat16)
    ok_ref[...] = got[:, wide : wide + HEAD].astype(jnp.bfloat16)
    ov_ref[...] = got[:, wide + HEAD :].astype(jnp.bfloat16)


def grad_qkv(at, pieces, dq, dkv, tile=512):
    rows, depth, wide = dkv.shape[0], pieces[0].shape[1], dq.shape[-1]
    shapes = [(depth, wide), (depth, HEAD), (depth, HEAD)]
    return pl.pallas_call(
        functools.partial(_dw_kernel, pieces=len(pieces)),
        grid_spec=pltpu.PrefetchScalarGridSpec(
            num_scalar_prefetch=1,
            grid=(depth // tile,),
            in_specs=[*(pl.BlockSpec(memory_space=pl.ANY) for _ in pieces), _whole(dq.shape), _whole(dkv.shape)],
            out_specs=[pl.BlockSpec((tile, t[1]), lambda i, at: (i, 0)) for t in shapes],
            scratch_shapes=[pltpu.VMEM((rows, wide + 2 * HEAD), jnp.bfloat16), pltpu.VMEM((2, rows, tile), jnp.bfloat16), pltpu.SemaphoreType.DMA((2,))],
        ),
        out_shape=[_like(t) for t in shapes],
        compiler_params=_params(),
        cost_estimate=_cost(2 * rows * depth * (wide + 2 * HEAD), [*pieces, dq, dkv]),
        name="grad_qkv",
    )(at, *pieces, dq, dkv)


def _dwo_kernel(at_ref, *refs, pieces):
    given, (out_ref, o_ref, rows_s, sem) = refs[:pieces], refs[pieces:]
    o_ref[...] = _dot(out_ref[...], _columns_here(at_ref, given, rows_s, sem), 0, 0).astype(jnp.bfloat16)


def grad_wo(at, pieces, out, tile=512):
    depth, (rows, wide) = pieces[0].shape[1], out.shape
    return pl.pallas_call(
        functools.partial(_dwo_kernel, pieces=len(pieces)),
        grid_spec=pltpu.PrefetchScalarGridSpec(
            num_scalar_prefetch=1,
            grid=(depth // tile,),
            in_specs=[*(pl.BlockSpec(memory_space=pl.ANY) for _ in pieces), _whole(out.shape)],
            out_specs=pl.BlockSpec((wide, tile), lambda i, at: (0, i)),
            scratch_shapes=[pltpu.VMEM((2, rows, tile), jnp.bfloat16), pltpu.SemaphoreType.DMA((2,))],
        ),
        out_shape=_like((wide, depth)),
        compiler_params=_params(),
        cost_estimate=_cost(2 * rows * depth * wide, [*pieces, out]),
        name="grad_wo",
    )(at, *pieces, out)


def _norm_kernel(*refs):
    x_ref, dy_ref, gain_ref, *das, o_ref, og_ref = refs
    x = x_ref[...].astype(jnp.float32)
    scale = lax.rsqrt(jnp.mean(x * x, -1, keepdims=True) + 1e-6)
    da = jnp.concatenate([r[...].astype(jnp.float32) for r in das], axis=1)
    unit = x * scale
    by_unit = da * gain_ref[...].astype(jnp.float32)
    mean = jnp.mean(by_unit * unit, -1, keepdims=True)
    o_ref[...] = (dy_ref[...].astype(jnp.float32) + scale * (by_unit - unit * mean)).astype(jnp.bfloat16)
    part = jnp.sum(da * unit, axis=0, keepdims=True)

    @pl.when(pl.program_id(0) == 0)
    def _():
        og_ref[...] = part

    @pl.when(pl.program_id(0) > 0)
    def _():
        og_ref[...] += part


def norm_bwd(x, dy, gain, das, tile=32):
    rows, depth = x.shape
    row = lambda n: pl.BlockSpec((tile, n), lambda i: (i, 0))
    return pl.pallas_call(
        _norm_kernel,
        grid=(rows // tile,),
        in_specs=[row(depth), row(depth), _whole((1, depth)), *(row(d.shape[1]) for d in das)],
        out_specs=[row(depth), pl.BlockSpec((1, depth), lambda i: (0, 0))],
        out_shape=[_like((rows, depth)), _like((1, depth), jnp.float32)],
        compiler_params=_params(),
        cost_estimate=_cost(20 * rows * depth, [x, dy, x, x]),
        name="norm_bwd",
    )(x, dy, gain.reshape(1, depth), *das)


def _share_kernel(n, mine_ref, o_ref, held, send_sem, recv_sem):
    me = lax.axis_index("tp")
    barrier = pltpu.get_barrier_semaphore()
    for d in range(1, n):
        pl.semaphore_signal(barrier, inc=1, device_id={"tp": lax.rem(me + d, n)}, device_id_type=pl.DeviceIdType.MESH)
    pl.semaphore_wait(barrier, n - 1)
    copies = []
    for d in range(1, n):
        copy = pltpu.make_async_remote_copy(src_ref=mine_ref, dst_ref=held.at[d - 1], send_sem=send_sem.at[d - 1], recv_sem=recv_sem.at[d - 1],
                                            device_id={"tp": lax.rem(me + d, n)}, device_id_type=pl.DeviceIdType.MESH)
        copy.start()
        copies.append(copy)
    for copy in copies:
        copy.wait()
    total = jnp.zeros(o_ref.shape, jnp.float32)
    for i in range(n):
        other = held[jnp.maximum(lax.rem(me - i + n, n) - 1, 0)]
        total += jnp.where(me == i, mine_ref[...], other)
    o_ref[...] = total


def share_sum(part, n):
    depth = part.shape[1]
    wide = part.reshape(8, depth // 8)
    return pl.pallas_call(
        functools.partial(_share_kernel, n),
        in_specs=[pl.BlockSpec(memory_space=pltpu.VMEM)],
        out_specs=pl.BlockSpec(memory_space=pltpu.VMEM),
        out_shape=_like(wide.shape, jnp.float32),
        scratch_shapes=[pltpu.VMEM((n - 1, *wide.shape), jnp.float32), pltpu.SemaphoreType.DMA((n - 1,)), pltpu.SemaphoreType.DMA((n - 1,))],
        compiler_params=pltpu.CompilerParams(collective_id=0, has_side_effects=True),
        cost_estimate=pl.CostEstimate(flops=n * depth, transcendentals=0, bytes_accessed=8 * depth),
        name="share_sum",
    )(wide).reshape(1, depth)


def solution(mesh):
    n = mesh.shape["tp"]
    chips = n // DEVS
    same = [list(range(c, n, DEVS)) for c in range(DEVS)]
    other = [(i, i ^ 1) for i in range(n)]
    right = [(i, (i + DEVS) % n) for i in range(n)]
    left = [(i, (i - DEVS) % n) for i in range(n)]

    def program(x, dy, gain, wq, wk, wv, wo):
        block, depth = x.shape
        rows = n * block
        span = block // PARTS
        me = lax.axis_index("tp")
        core, chip = lax.rem(me, DEVS), lax.div(me, DEVS)

        def send(t, ring):
            return lax.ppermute(t, "tp", ring)

        places = lambda *steps: jnp.stack([jnp.stack([lax.rem(chip + shift, chips), jnp.full_like(chip, half)]) for shift, half in steps])
        tables = [places((0, 0), (0, 1)), places((chips - 1, 0), (1, 1)), places((chips - 1, 1), (1, 0)), places((2, 0), (2, 1))]

        def gather(t):
            top, low = t[:span], t[span:]
            from_left0, from_right1 = send(top, right), send(low, left)
            from_left1, from_right0 = send(low, right), send(top, left)
            across0, across1 = send(from_left0, right), send(from_right1, left)
            groups = [(top, low), (from_left0, from_right1), (from_left1, from_right0), (across0, across1)]
            return [(*g, *(send(p, other) for p in g)) for g in groups]

        near = jnp.stack([core * span, block + core * span, (1 - core) * span, block + (1 - core) * span])
        far = jnp.concatenate([jnp.concatenate([(t[:, 0] * DEVS + c) * block + t[:, 1] * span for c in (core, 1 - core)]) for t in tables])

        half = HEAD // 2
        angle = jnp.arange(rows, dtype=jnp.float32)[:, None] * THETA ** (-jnp.arange(half, dtype=jnp.float32) / half)
        cos, sin = jnp.cos(angle), jnp.sin(angle)
        cos, sin = (jnp.concatenate(t, 1).reshape(n, PARTS, span, HEAD) for t in ([cos, cos], [-sin, sin]))

        xs = gather(normed(x, gain))
        dys = gather(dy)
        w = jnp.concatenate([wq, wk, wv], axis=1)
        pw = send(w, other)
        got = None
        for table, pieces in zip(tables, xs):
            got = qkv(table, near, pieces, w, cos, sin, got)
        q, k, v = got
        k, v = k.reshape(rows, HEAD), v.reshape(rows, HEAD)
        out, lse = attend(q, k, v)
        got = None
        for i, (table, pieces) in enumerate(zip(tables, dys)):
            d_out = back_through_wo(near, pieces, wo)
            got = attend_bwd(table, q, k, v, d_out, out, lse, cos, sin, got, i == len(dys) - 1)
        dq, dkv = got
        dkvs = dkv.reshape(chips, DEVS, block, 2 * HEAD)
        pq = send(lax.dynamic_index_in_dim(dq, 1 - core, 0, False), other)
        pkv = send(lax.dynamic_index_in_dim(dkvs, 1 - core, 1, False), other)
        width = depth // COLS
        das = []
        for c in range(COLS):
            term = grad_a(core[None], dq, dkvs, pq, pkv, w, pw, c * width, width)
            das.append(lax.psum_scatter(term, "tp", scatter_dimension=0, axis_index_groups=same, tiled=True))
        flat = lambda groups: [p for g in groups for p in g]
        by_wo = grad_wo(far, flat(dys), out.reshape(rows, -1))
        by_qkv = grad_qkv(far, flat(xs), dq, dkv)
        by_x, by_gain = norm_bwd(x, dy, gain, das)
        return by_x, share_sum(by_gain, n), *by_qkv, by_wo

    tokens, columns = P(("dp", "tp"), None), P(None, "tp")
    return jax.shard_map(
        program,
        mesh=mesh,
        in_specs=(tokens, tokens, P(None), columns, columns, columns, P("tp", None)),
        out_specs=(tokens, P("dp", None), P("dp", "tp"), P("dp", "tp"), P("dp", "tp"), P(("dp", "tp"), None)),
        check_vma=False,
    )
```

```python
import functools

import jax
import jax.numpy as jnp
from jax import lax
from jax.experimental import pallas as pl
from jax.experimental.pallas import tpu as pltpu
from jax.sharding import PartitionSpec as P


NEG = -1e30
HIDDEN = 2 * NEG
LOG2E = 1.4426950408889634
VMEM = 62 * 2**20
HEAD = 128
THETA = 10000
PARTS = 2
DEVS = 2
BK = 512
COLS = 3, 11


def _dot(a, b, ca, cb):
    return lax.dot_general(a, b, (((ca,), (cb,)), ((), ())), preferred_element_type=jnp.float32)


def _whole(shape):
    return pl.BlockSpec(shape, lambda *_: (0,) * len(shape), pipeline_mode=pl.Buffered(1))


def _params(n=1):
    return pltpu.CompilerParams(dimension_semantics=("arbitrary",) * n, vmem_limit_bytes=VMEM)


def _cost(flops, arrays, exps=0):
    return pl.CostEstimate(flops=int(flops), transcendentals=int(exps), bytes_accessed=sum(a.size * a.dtype.itemsize for a in arrays))


def _like(shape, dtype=jnp.bfloat16):
    return jax.ShapeDtypeStruct(shape, dtype)


def _normed_kernel(x_ref, y_ref, gain_ref, *outs):
    for ref, o_ref in zip((x_ref, y_ref), outs):
        wide = ref[...].astype(jnp.float32)
        scale = lax.rsqrt(jnp.mean(wide * wide, -1, keepdims=True) + 1e-6)
        o_ref[...] = (wide * scale * gain_ref[...].astype(jnp.float32)).astype(jnp.bfloat16)


def normed(x, gain, tile=32):
    rows, depth = x.shape
    steps = rows // 2 // tile
    row = lambda skip: pl.BlockSpec((tile, depth), lambda i: (i + skip, 0))
    return pl.pallas_call(
        _normed_kernel,
        grid=(steps,),
        in_specs=[row(0), row(steps), _whole((1, depth))],
        out_specs=[row(0)] * 2,
        out_shape=[_like((rows // 2, depth))] * 2,
        compiler_params=_params(),
        cost_estimate=_cost(6 * rows * depth, [x, x]),
        name="normed",
    )(x, x, gain.reshape(1, depth))


def _turn(t, cos, sin):
    t = t.astype(jnp.bfloat16).astype(jnp.float32)
    return (t * cos + pltpu.roll(t, HEAD // 2, 1) * sin).astype(jnp.bfloat16)


def _fetch(at_ref, pieces, rows_s, sem, columns=None):
    copies = []
    for n, piece in enumerate(pieces):
        rows = piece.shape[0]
        place = rows_s.at[pl.ds(pl.multiple_of(at_ref[n], rows), rows)]
        copies.append(pltpu.make_async_copy(piece if columns is None else piece.at[:, columns], place, sem))
    return copies


def _gathered(at_ref, given, rows_s):
    for n, ref in enumerate(given):
        rows_s[pl.ds(pl.multiple_of(at_ref[n], ref.shape[0]), ref.shape[0]), :] = ref[...]
    return rows_s[...]


def _add(acc, here, got):
    @pl.when(pl.program_id(0) == 0)
    def _():
        acc[:, here] = got

    @pl.when(pl.program_id(0) > 0)
    def _():
        acc[:, here] += got


def _qkv_kernel(table_ref, at_ref, *refs, pieces, carried):
    given, (wq_ref, wk_ref, wv_ref, cos_ref, sin_ref, *refs) = refs[:pieces], refs[pieces:]
    q_ref, k_ref, v_ref, rows_s, acc, q_s, k_s, v_s, sem = refs[carried:]
    wide = wq_ref.shape[1]
    rows = _gathered(at_ref, given, rows_s)
    _add(acc, slice(0, wide), _dot(rows, wq_ref[...], 1, 0))
    _add(acc, slice(wide, wide + 2 * HEAD), _dot(rows, jnp.concatenate([wk_ref[...], wv_ref[...]], axis=1), 1, 0))

    @pl.when(pl.program_id(0) == pl.num_programs(0) - 1)
    def _():
        steps, devices, span, _ = q_s.shape
        copies = []
        for i in range(steps):
            chip, half = table_ref[i, 0], table_ref[i, 1]
            to = (pl.ds(chip * devices, devices), half)
            for d in range(devices):
                here = slice((i * devices + d) * span, (i * devices + d + 1) * span)
                cos, sin = cos_ref[chip * devices + d, half], sin_ref[chip * devices + d, half]
                for h in range(0, wide, HEAD):
                    q_s[i, d, :, h : h + HEAD] = _turn(acc[here, h : h + HEAD], cos, sin)
                k_s[i, d] = _turn(acc[here, wide : wide + HEAD], cos, sin)
                v_s[i, d] = acc[here, wide + HEAD :].astype(jnp.bfloat16)
            for n, (scratch, ref) in enumerate(((q_s, q_ref), (k_s, k_ref), (v_s, v_ref))):
                copies.append(pltpu.make_async_copy(scratch.at[i], ref.at[to], sem.at[i, n]))
                copies[-1].start()
        for copy in copies:
            copy.wait()


def _step_spec(span, wide):
    return pl.BlockSpec((DEVS, 1, span, wide), lambda i, table, *_: (table[i, 0], table[i, 1], 0, 0))


def qkv(table, at, pieces, weights, cos, sin, sofar, chunks=4):
    devices, parts, span, _ = cos.shape
    depth = weights[0].shape[0]
    widths = [t.shape[1] for t in weights]
    steps, tile = table.shape[0], depth // chunks
    rows = steps * DEVS * span
    sofar = sofar or ()
    any_ = pl.BlockSpec(memory_space=pl.ANY)
    return pl.pallas_call(
        functools.partial(_qkv_kernel, pieces=len(pieces), carried=len(sofar)),
        grid_spec=pltpu.PrefetchScalarGridSpec(
            num_scalar_prefetch=2,
            grid=(chunks,),
            in_specs=[*(pl.BlockSpec((t.shape[0], tile), lambda i, *_: (0, i)) for t in pieces), *(pl.BlockSpec((tile, n), lambda i, *_: (i, 0)) for n in widths),
                      _whole(cos.shape), _whole(sin.shape), *(any_ for _ in sofar)],
            out_specs=[any_ for _ in widths],
            scratch_shapes=[pltpu.VMEM((rows, tile), jnp.bfloat16), pltpu.VMEM((rows, sum(widths)), jnp.float32),
                            *(pltpu.VMEM((steps, DEVS, span, n), jnp.bfloat16) for n in widths), pltpu.SemaphoreType.DMA((steps, len(widths)))],
        ),
        out_shape=[_like((devices, parts, span, n)) for n in widths],
        input_output_aliases={2 + len(pieces) + len(widths) + 2 + n: n for n in range(len(sofar))},
        compiler_params=_params(),
        cost_estimate=pl.CostEstimate(flops=2 * rows * depth * sum(widths), transcendentals=0, bytes_accessed=2 * depth * (rows + sum(widths))),
        name="qkv",
    )(table, at, *pieces, *weights, cos, sin, *sofar)


def _wo_kernel(at_ref, *refs, pieces):
    given, (w_ref, o_ref, rows_s, acc) = refs[:pieces], refs[pieces:]
    _add(acc, slice(None), _dot(_gathered(at_ref, given, rows_s), w_ref[...], 1, 1))

    @pl.when(pl.program_id(0) == pl.num_programs(0) - 1)
    def _():
        o_ref[...] = acc[...].astype(jnp.bfloat16)


def back_through_wo(at, pieces, wo, chunks=4):
    rows, (wide, depth) = sum(p.shape[0] for p in pieces), wo.shape
    tile = depth // chunks
    return pl.pallas_call(
        functools.partial(_wo_kernel, pieces=len(pieces)),
        grid_spec=pltpu.PrefetchScalarGridSpec(
            num_scalar_prefetch=1,
            grid=(chunks,),
            in_specs=[*(pl.BlockSpec((t.shape[0], tile), lambda i, at: (0, i)) for t in pieces), pl.BlockSpec((wide, tile), lambda i, at: (0, i))],
            out_specs=_whole((rows, wide)),
            scratch_shapes=[pltpu.VMEM((rows, tile), jnp.bfloat16), pltpu.VMEM((rows, wide), jnp.float32)],
        ),
        out_shape=_like((rows, wide)),
        compiler_params=_params(),
        cost_estimate=pl.CostEstimate(flops=2 * rows * depth * wide, transcendentals=0, bytes_accessed=2 * depth * (rows + wide)),
        name="back_through_wo",
    )(at, *pieces, wo)


def _gaps(span):
    column = lax.broadcasted_iota(jnp.int32, (BK, DEVS * span), 1)
    place = (column // span) * (span * PARTS) + column % span
    return place - lax.broadcasted_iota(jnp.int32, (BK, DEVS * span), 0)


def _part(ref, h):
    return ref[:, 0, :, h * HEAD : (h + 1) * HEAD].reshape(-1, HEAD)


def _forward(q_ref, k_ref, v_ref, o_ref, lse_ref, top_s, mix_s, gap_s):
    chip, half = pl.program_id(0), pl.program_id(1)
    span = q_ref.shape[2]
    heads = q_ref.shape[-1] // HEAD
    scale = HEAD**-0.5
    e = scale * LOG2E

    @pl.when((chip == 0) & (half == 0))
    def _():
        gap_s[...] = _gaps(span)

    top_s[...] = jnp.full(top_s.shape, NEG, jnp.float32)
    mix_s[...] = jnp.zeros(mix_s.shape, jnp.float32)

    def step(j, masked):
        here = pl.ds(pl.multiple_of(j * BK, BK), BK)
        k = k_ref[here, :]
        values = jnp.concatenate([v_ref[here, :].T, jnp.ones((8, BK), jnp.bfloat16)], axis=0)
        scores = [_dot(k, _part(q_ref, h), 1, 1) for h in range(heads)]
        weights, keeps = [], []
        for h, s in enumerate(scores):
            if masked:
                s = jnp.where(gap_s[...] >= -half * span, s, HIDDEN)
            old = top_s[h : h + 1, :]
            top = jnp.maximum(old, s.max(axis=0, keepdims=True))
            top_s[h : h + 1, :] = top
            weights.append(jnp.exp2((s - top) * e).astype(jnp.bfloat16))
            keeps.append(jnp.exp2((old - top) * e))
        for h in range(heads):
            mix_s[h] = mix_s[h] * keeps[h] + _dot(values, weights[h], 1, 0)

    lax.fori_loop(0, chip, lambda j, _: step(j, False), None)
    step(chip, True)
    for h in range(heads):
        total = mix_s[h, HEAD : HEAD + 1, :]
        o_ref[:, 0, :, h * HEAD : (h + 1) * HEAD] = (mix_s[h, :HEAD, :] * (1 / total)).T.astype(jnp.bfloat16).reshape(DEVS, span, HEAD)
        lse_ref[0, 0, h : h + 1, :] = top_s[h : h + 1, :] * scale + jnp.log(total)


def attend(q, k, v):
    devices, parts, span, wide = q.shape
    heads, nq, keys = wide // HEAD, DEVS * span, k.shape[0]
    chips = devices // DEVS
    part = pl.BlockSpec((DEVS, 1, span, wide), lambda i, j: (i, j, 0, 0))
    return pl.pallas_call(
        _forward,
        grid=(chips, parts),
        in_specs=[part, _whole(k.shape), _whole(v.shape)],
        out_specs=[part, pl.BlockSpec((1, 1, heads, nq), lambda i, j: (i, j, 0, 0))],
        out_shape=[_like(q.shape), _like((chips, parts, heads, nq), jnp.float32)],
        scratch_shapes=[pltpu.VMEM((heads, nq), jnp.float32), pltpu.VMEM((heads, HEAD + 8, nq), jnp.float32), pltpu.VMEM((BK, nq), jnp.int32)],
        compiler_params=_params(2),
        cost_estimate=_cost(2 * q.size * keys * 2, [q, k, v, q], q.size // HEAD * keys),
        name="attend",
    )(q, k, v)


def _backward(table_ref, *refs, first, last):
    q_ref, k_ref, v_ref, do_ref, o_ref, lse_ref, cos_ref, sin_ref, *refs = refs
    if not first:
        dk_in, dv_in, _, *refs = refs
    if last:
        kcos_ref, ksin_ref, dq_ref, dkv_ref, *refs = refs
    else:
        dq_ref, dk_ref, dv_ref, *refs = refs
    dq_s, dk_s, dv_s, gap_s = refs
    i = pl.program_id(0)
    chip, half = table_ref[i, 0], table_ref[i, 1]
    span = q_ref.shape[2]
    heads = q_ref.shape[-1] // HEAD
    scale = HEAD**-0.5
    e = scale * LOG2E

    @pl.when(i == 0)
    def _():
        gap_s[...] = _gaps(span)
        dk_s[...] = jnp.zeros(dk_s.shape, jnp.float32) if first else dk_in[...]
        dv_s[...] = jnp.zeros(dv_s.shape, jnp.float32) if first else dv_in[...]

    dq_s[...] = jnp.zeros(dq_s.shape, jnp.float32)
    head = lambda ref, h: ref[:, h * HEAD : (h + 1) * HEAD]
    lses = [lse_ref[0, 0, h : h + 1, :] * LOG2E for h in range(heads)]
    deltas = [(head(do_ref, h).astype(jnp.float32) * _part(o_ref, h).astype(jnp.float32)).T.sum(axis=0, keepdims=True) for h in range(heads)]

    def step(j, masked):
        here = pl.ds(pl.multiple_of(j * BK, BK), BK)
        k, v = k_ref[here, :], v_ref[here, :]
        kt = k.T
        scores = [_dot(k, _part(q_ref, h), 1, 1) for h in range(heads)]
        dps = [_dot(v, head(do_ref, h), 1, 1) for h in range(heads)]
        for h in range(heads):
            w = jnp.exp2(scores[h] * e - lses[h])
            if masked:
                w = jnp.where(gap_s[...] >= -half * span, w, 0.0)
            ds = (w * (dps[h] - deltas[h])).astype(jnp.bfloat16)
            dv_s[here, :] += _dot(w.astype(jnp.bfloat16), head(do_ref, h), 1, 0)
            dk_s[here, :] += _dot(ds, _part(q_ref, h), 1, 0)
            dq_s[h] += _dot(kt, ds, 1, 0)

    lax.fori_loop(0, chip, lambda j, _: step(j, False), None)
    step(chip, True)
    cos, sin = (r[:, 0].reshape(-1, HEAD) for r in (cos_ref, sin_ref))
    for h in range(heads):
        dq_ref[:, 0, 0, :, h * HEAD : (h + 1) * HEAD] = _turn((dq_s[h] * scale).T, cos, -sin).reshape(DEVS, span, HEAD)

    @pl.when(i == pl.num_programs(0) - 1)
    def _():
        if last:
            dkv_ref[:, :HEAD] = _turn(dk_s[...] * scale, kcos_ref[...], -ksin_ref[...])
            dkv_ref[:, HEAD:] = dv_s[...].astype(jnp.bfloat16)
        else:
            dk_ref[...] = dk_s[...]
            dv_ref[...] = dv_s[...]


def attend_bwd(table, q, k, v, d_out, out, lse, cos, sin, sofar, last):
    devices, parts, span, wide = q.shape
    heads, nq, keys = wide // HEAD, DEVS * span, k.shape[0]
    chips = devices // DEVS
    steps = table.shape[0]
    kv = _whole(k.shape)
    dq_shape = (DEVS, chips, parts, span, wide)
    more, specs = [], []
    if sofar is not None:
        dq, dk, dv = sofar
        more, specs = [dk, dv, dq], [kv, kv, pl.BlockSpec(memory_space=pl.ANY)]
    if last:
        more, specs = [*more, cos.reshape(keys, HEAD), sin.reshape(keys, HEAD)], [*specs, kv, kv]
    sums = [(keys, 2 * HEAD)] if last else [k.shape, k.shape]
    return pl.pallas_call(
        functools.partial(_backward, first=sofar is None, last=last),
        grid_spec=pltpu.PrefetchScalarGridSpec(
            num_scalar_prefetch=1,
            grid=(steps,),
            in_specs=[_step_spec(span, wide), kv, kv, pl.BlockSpec((nq, wide), lambda i, table: (i, 0)), _step_spec(span, wide),
                      pl.BlockSpec((1, 1, heads, nq), lambda i, table: (table[i, 0], table[i, 1], 0, 0)),
                      _step_spec(span, HEAD), _step_spec(span, HEAD), *specs],
            out_specs=[pl.BlockSpec((DEVS, 1, 1, span, wide), lambda i, table: (0, table[i, 0], table[i, 1], 0, 0)), *(_whole(t) for t in sums)],
            scratch_shapes=[pltpu.VMEM((heads, HEAD, nq), jnp.float32), pltpu.VMEM((keys, HEAD), jnp.float32),
                            pltpu.VMEM((keys, HEAD), jnp.float32), pltpu.VMEM((BK, nq), jnp.int32)],
        ),
        out_shape=[_like(dq_shape), *(_like(t, jnp.bfloat16 if last else jnp.float32) for t in sums)],
        input_output_aliases={} if sofar is None else {11: 0},
        compiler_params=_params(),
        cost_estimate=pl.CostEstimate(flops=2 * steps * nq * wide * keys * 5, transcendentals=steps * nq * heads * keys, bytes_accessed=8 * steps * nq * wide),
        name="attend_bwd",
    )(table, q, k, v, d_out, out, lse, cos, sin, *more)


def _da_kernel(core_ref, dq_ref, dkv_ref, pq_ref, pkv_ref, wq_ref, wk_ref, wv_ref, pwq_ref, pwk_ref, pwv_ref, o_ref, kv_s):
    chips, parts, span, wide = pq_ref.shape
    rows = chips * parts * span

    @pl.when(pl.program_id(0) == 0)
    def _():
        kv_s[:, : 2 * HEAD] = dkv_ref[:, 0].reshape(rows, 2 * HEAD)
        kv_s[:, 2 * HEAD :] = pkv_ref[...].reshape(rows, 2 * HEAD)

    wkv = jnp.concatenate([r[...] for r in (wk_ref, wv_ref, pwk_ref, pwv_ref)], axis=1)
    got = _dot(dq_ref[0].reshape(rows, wide), wq_ref[...], 1, 1) + _dot(pq_ref[...].reshape(rows, wide), pwq_ref[...], 1, 1)
    o_ref[...] = (got + _dot(kv_s[...], wkv, 1, 1)).astype(jnp.bfloat16)


def grad_a(core, dq, dkv, pq, pkv, weights, others, first, columns, tile=512):
    chips, parts, span, wide = pq.shape
    block = parts * span
    rows = chips * block
    skip = first // tile
    once = dict(pipeline_mode=pl.Buffered(1))
    return pl.pallas_call(
        _da_kernel,
        grid_spec=pltpu.PrefetchScalarGridSpec(
            num_scalar_prefetch=1,
            grid=(columns // tile,),
            in_specs=[pl.BlockSpec((1, chips, parts, span, wide), lambda i, core: (core[0], 0, 0, 0, 0), **once),
                      pl.BlockSpec((chips, 1, block, 2 * HEAD), lambda i, core: (0, core[0], 0, 0), **once),
                      _whole(pq.shape), _whole(pkv.shape), *(pl.BlockSpec((tile, t.shape[1]), lambda i, core: (i + skip, 0)) for t in (*weights, *others))],
            out_specs=pl.BlockSpec((rows, tile), lambda i, core: (0, i)),
            scratch_shapes=[pltpu.VMEM((rows, 4 * HEAD), jnp.bfloat16)],
        ),
        out_shape=_like((rows, columns)),
        compiler_params=_params(),
        cost_estimate=pl.CostEstimate(flops=4 * rows * columns * (wide + 2 * HEAD), transcendentals=0, bytes_accessed=4 * columns * (wide + 2 * HEAD)),
        name="grad_a",
    )(core, dq, dkv, pq, pkv, *weights, *others)


def _columns_here(at_ref, pieces, rows_s, sem):
    i, steps = pl.program_id(0), pl.num_programs(0)
    tile = rows_s.shape[-1]

    def copies(step):
        slot = lax.rem(step, 2)
        return _fetch(at_ref, pieces, rows_s.at[slot], sem.at[slot], pl.ds(pl.multiple_of(step * tile, tile), tile))

    @pl.when(i == 0)
    def _():
        for copy in copies(i):
            copy.start()

    @pl.when(i + 1 < steps)
    def _():
        for copy in copies(i + 1):
            copy.start()

    for copy in copies(i):
        copy.wait()
    return rows_s[lax.rem(i, 2)]


def _dw_kernel(at_ref, *refs, pieces):
    given, (dq_ref, dkv_ref, oq_ref, ok_ref, ov_ref, cat_s, rows_s, sem) = refs[:pieces], refs[pieces:]
    wide = oq_ref.shape[1]

    @pl.when(pl.program_id(0) == 0)
    def _():
        cat_s[:, wide:] = dkv_ref[...]
        cores, chips, parts, span, _ = dq_ref.shape
        for chip in range(chips):
            for core in range(cores):
                for n in range(parts):
                    at = ((chip * cores + core) * parts + n) * span
                    cat_s[at : at + span, :wide] = dq_ref[core, chip, n]

    got = _dot(_columns_here(at_ref, given, rows_s, sem), cat_s[...], 0, 0)
    oq_ref[...] = got[:, :wide].astype(jnp.bfloat16)
    ok_ref[...] = got[:, wide : wide + HEAD].astype(jnp.bfloat16)
    ov_ref[...] = got[:, wide + HEAD :].astype(jnp.bfloat16)


def grad_qkv(at, pieces, dq, dkv, tile=512):
    rows, depth, wide = dkv.shape[0], pieces[0].shape[1], dq.shape[-1]
    shapes = [(depth, wide), (depth, HEAD), (depth, HEAD)]
    return pl.pallas_call(
        functools.partial(_dw_kernel, pieces=len(pieces)),
        grid_spec=pltpu.PrefetchScalarGridSpec(
            num_scalar_prefetch=1,
            grid=(depth // tile,),
            in_specs=[*(pl.BlockSpec(memory_space=pl.ANY) for _ in pieces), _whole(dq.shape), _whole(dkv.shape)],
            out_specs=[pl.BlockSpec((tile, t[1]), lambda i, at: (i, 0)) for t in shapes],
            scratch_shapes=[pltpu.VMEM((rows, wide + 2 * HEAD), jnp.bfloat16), pltpu.VMEM((2, rows, tile), jnp.bfloat16), pltpu.SemaphoreType.DMA((2,))],
        ),
        out_shape=[_like(t) for t in shapes],
        compiler_params=_params(),
        cost_estimate=_cost(2 * rows * depth * (wide + 2 * HEAD), [*pieces, dq, dkv]),
        name="grad_qkv",
    )(at, *pieces, dq, dkv)


def _dwo_kernel(at_ref, *refs, pieces):
    given, (out_ref, o_ref, rows_s, sem) = refs[:pieces], refs[pieces:]
    o_ref[...] = _dot(out_ref[...], _columns_here(at_ref, given, rows_s, sem), 0, 0).astype(jnp.bfloat16)


def grad_wo(at, pieces, out, tile=512):
    depth, (rows, wide) = pieces[0].shape[1], out.shape
    return pl.pallas_call(
        functools.partial(_dwo_kernel, pieces=len(pieces)),
        grid_spec=pltpu.PrefetchScalarGridSpec(
            num_scalar_prefetch=1,
            grid=(depth // tile,),
            in_specs=[*(pl.BlockSpec(memory_space=pl.ANY) for _ in pieces), _whole(out.shape)],
            out_specs=pl.BlockSpec((wide, tile), lambda i, at: (0, i)),
            scratch_shapes=[pltpu.VMEM((2, rows, tile), jnp.bfloat16), pltpu.SemaphoreType.DMA((2,))],
        ),
        out_shape=_like((wide, depth)),
        compiler_params=_params(),
        cost_estimate=_cost(2 * rows * depth * wide, [*pieces, out]),
        name="grad_wo",
    )(at, *pieces, out)


def _norm_kernel(*refs):
    x_ref, dy_ref, gain_ref, *das, o_ref, og_ref = refs
    x = x_ref[...].astype(jnp.float32)
    scale = lax.rsqrt(jnp.mean(x * x, -1, keepdims=True) + 1e-6)
    da = jnp.concatenate([r[...].astype(jnp.float32) for r in das], axis=1)
    unit = x * scale
    by_unit = da * gain_ref[...].astype(jnp.float32)
    mean = jnp.mean(by_unit * unit, -1, keepdims=True)
    o_ref[...] = (dy_ref[...].astype(jnp.float32) + scale * (by_unit - unit * mean)).astype(jnp.bfloat16)
    part = jnp.sum(da * unit, axis=0, keepdims=True)

    @pl.when(pl.program_id(0) == 0)
    def _():
        og_ref[...] = part

    @pl.when(pl.program_id(0) > 0)
    def _():
        og_ref[...] += part


def norm_bwd(x, dy, gain, das, tile=64):
    rows, depth = x.shape
    row = lambda n: pl.BlockSpec((tile, n), lambda i: (i, 0))
    return pl.pallas_call(
        _norm_kernel,
        grid=(rows // tile,),
        in_specs=[row(depth), row(depth), _whole((1, depth)), *(row(d.shape[1]) for d in das)],
        out_specs=[row(depth), pl.BlockSpec((1, depth), lambda i: (0, 0))],
        out_shape=[_like((rows, depth)), _like((1, depth), jnp.float32)],
        compiler_params=_params(),
        cost_estimate=_cost(20 * rows * depth, [x, dy, x, x]),
        name="norm_bwd",
    )(x, dy, gain.reshape(1, depth), *das)


def _share_kernel(n, mine_ref, o_ref, held, send_sem, recv_sem):
    me = lax.axis_index("tp")
    barrier = pltpu.get_barrier_semaphore()
    for d in range(1, n):
        pl.semaphore_signal(barrier, inc=1, device_id={"tp": lax.rem(me + d, n)}, device_id_type=pl.DeviceIdType.MESH)
    pl.semaphore_wait(barrier, n - 1)
    copies = []
    for d in range(1, n):
        copy = pltpu.make_async_remote_copy(src_ref=mine_ref, dst_ref=held.at[d - 1], send_sem=send_sem.at[d - 1], recv_sem=recv_sem.at[d - 1],
                                            device_id={"tp": lax.rem(me + d, n)}, device_id_type=pl.DeviceIdType.MESH)
        copy.start()
        copies.append(copy)
    for copy in copies:
        copy.wait()
    total = jnp.zeros(o_ref.shape, jnp.float32)
    for i in range(n):
        other = held[jnp.maximum(lax.rem(me - i + n, n) - 1, 0)]
        total += jnp.where(me == i, mine_ref[...], other)
    o_ref[...] = total


def share_sum(part, n):
    return pl.pallas_call(
        functools.partial(_share_kernel, n),
        in_specs=[pl.BlockSpec(memory_space=pltpu.VMEM)],
        out_specs=pl.BlockSpec(memory_space=pltpu.VMEM),
        out_shape=_like(part.shape, jnp.float32),
        scratch_shapes=[pltpu.VMEM((n - 1, *part.shape), jnp.float32), pltpu.SemaphoreType.DMA((n - 1,)), pltpu.SemaphoreType.DMA((n - 1,))],
        compiler_params=pltpu.CompilerParams(collective_id=0, has_side_effects=True),
        cost_estimate=pl.CostEstimate(flops=n * part.size, transcendentals=0, bytes_accessed=8 * part.size),
        name="share_sum",
    )(part)


def solution(mesh):
    n = mesh.shape["tp"]
    chips = n // DEVS
    same = [list(range(c, n, DEVS)) for c in range(DEVS)]
    other = [(i, i ^ 1) for i in range(n)]
    right = [(i, (i + DEVS) % n) for i in range(n)]
    left = [(i, (i - DEVS) % n) for i in range(n)]

    def program(x, dy, gain, wq, wk, wv, wo):
        block, depth = x.shape
        rows = n * block
        span = block // PARTS
        me = lax.axis_index("tp")
        core, chip = lax.rem(me, DEVS), lax.div(me, DEVS)

        def send(t, ring):
            return lax.ppermute(t, "tp", ring)

        places = lambda *steps: jnp.stack([jnp.stack([lax.rem(chip + shift, chips), jnp.full_like(chip, half)]) for shift, half in steps])
        tables = [places((0, 0), (0, 1)), places((chips - 1, 0), (1, 1)), places((chips - 1, 1), (1, 0)), places((2, 0), (2, 1))]

        def gather(t):
            top, low = t
            from_left0, from_right1 = send(top, right), send(low, left)
            from_left1, from_right0 = send(low, right), send(top, left)
            across0, across1 = send(from_left0, right), send(from_right1, left)
            groups = [(top, low), (from_left0, from_right1), (from_left1, from_right0), (across0, across1)]
            return [(*g, *(send(p, other) for p in g)) for g in groups]

        near = jnp.stack([core * span, block + core * span, (1 - core) * span, block + (1 - core) * span])
        far = jnp.concatenate([jnp.concatenate([(t[:, 0] * DEVS + c) * block + t[:, 1] * span for c in (core, 1 - core)]) for t in tables])

        half = HEAD // 2
        angle = jnp.arange(rows, dtype=jnp.float32)[:, None] * THETA ** (-jnp.arange(half, dtype=jnp.float32) / half)
        cos, sin = jnp.cos(angle), jnp.sin(angle)
        cos, sin = lax.optimization_barrier((jnp.concatenate([cos, cos], 1), jnp.concatenate([-sin, sin], 1)))
        cos, sin = (t.reshape(n, PARTS, span, HEAD) for t in (cos, sin))

        xs = gather(normed(x, gain))
        dys = gather((dy[:span], dy[span:]))
        weights = wq, wk, wv
        others = [send(t, other) for t in weights]
        got = None
        for table, pieces in zip(tables, xs):
            got = qkv(table, near, pieces, weights, cos, sin, got)
        q, k, v = got
        k, v = k.reshape(rows, HEAD), v.reshape(rows, HEAD)
        out, lse = attend(q, k, v)
        got = None
        for i, (table, pieces) in enumerate(zip(tables, dys)):
            d_out = back_through_wo(near, pieces, wo)
            got = attend_bwd(table, q, k, v, d_out, out, lse, cos, sin, got, i == len(dys) - 1)
        dq, dkv = got
        dkvs = dkv.reshape(chips, DEVS, block, 2 * HEAD)
        pq = send(lax.dynamic_index_in_dim(dq, 1 - core, 0, False), other)
        pkv = send(lax.dynamic_index_in_dim(dkvs, 1 - core, 1, False), other)
        das, first = [], 0
        for share in COLS:
            width = depth * share // sum(COLS)
            term = grad_a(core[None], dq, dkvs, pq, pkv, weights, others, first, width)
            first += width
            das.append(lax.psum_scatter(term, "tp", scatter_dimension=0, axis_index_groups=same, tiled=True))
        flat = lambda groups: [p for g in groups for p in g]
        by_wo = grad_wo(far, flat(dys), out.reshape(rows, -1))
        by_qkv = grad_qkv(far, flat(xs), dq, dkv)
        by_x, by_gain = norm_bwd(x, dy, gain, das)
        return by_x, share_sum(by_gain, n), *by_qkv, by_wo

    tokens, columns = P(("dp", "tp"), None), P(None, "tp")
    return jax.shard_map(
        program,
        mesh=mesh,
        in_specs=(tokens, tokens, P(None), columns, columns, columns, P("tp", None)),
        out_specs=(tokens, P("dp", None), P("dp", "tp"), P("dp", "tp"), P("dp", "tp"), P(("dp", "tp"), None)),
        check_vma=False,
    )
```

```python
import functools

import jax
import jax.numpy as jnp
from jax import lax
from jax.experimental import pallas as pl
from jax.experimental.pallas import tpu as pltpu
from jax.sharding import PartitionSpec as P


NEG = -1e30
HIDDEN = 2 * NEG
LOG2E = 1.4426950408889634
VMEM = 62 * 2**20
HEAD = 128
THETA = 10000
PARTS = 2
DEVS = 2
BK = 512
COLS = 3, 11


def _dot(a, b, ca, cb):
    return lax.dot_general(a, b, (((ca,), (cb,)), ((), ())), preferred_element_type=jnp.float32)


def _whole(shape):
    return pl.BlockSpec(shape, lambda *_: (0,) * len(shape), pipeline_mode=pl.Buffered(1))


def _params(n=1):
    return pltpu.CompilerParams(dimension_semantics=("arbitrary",) * n, vmem_limit_bytes=VMEM)


def _cost(flops, arrays, exps=0):
    return pl.CostEstimate(flops=int(flops), transcendentals=int(exps), bytes_accessed=sum(a.size * a.dtype.itemsize for a in arrays))


def _like(shape, dtype=jnp.bfloat16):
    return jax.ShapeDtypeStruct(shape, dtype)


def _normed_kernel(x_ref, y_ref, gain_ref, *outs):
    for ref, o_ref in zip((x_ref, y_ref), outs):
        wide = ref[...].astype(jnp.float32)
        scale = lax.rsqrt(jnp.mean(wide * wide, -1, keepdims=True) + 1e-6)
        o_ref[...] = (wide * scale * gain_ref[...].astype(jnp.float32)).astype(jnp.bfloat16)


def normed(x, gain, tile=32):
    rows, depth = x.shape
    steps = rows // 2 // tile
    row = lambda skip: pl.BlockSpec((tile, depth), lambda i: (i + skip, 0))
    return pl.pallas_call(
        _normed_kernel,
        grid=(steps,),
        in_specs=[row(0), row(steps), _whole((1, depth))],
        out_specs=[row(0)] * 2,
        out_shape=[_like((rows // 2, depth))] * 2,
        compiler_params=_params(),
        cost_estimate=_cost(6 * rows * depth, [x, x]),
        name="normed",
    )(x, x, gain.reshape(1, depth))


def _turn(t, cos, sin):
    t = t.astype(jnp.bfloat16).astype(jnp.float32)
    return (t * cos + pltpu.roll(t, HEAD // 2, 1) * sin).astype(jnp.bfloat16)


def _fetch(at_ref, pieces, rows_s, sem, columns=None):
    copies = []
    for n, piece in enumerate(pieces):
        rows = piece.shape[0]
        place = rows_s.at[pl.ds(pl.multiple_of(at_ref[n], rows), rows)]
        copies.append(pltpu.make_async_copy(piece if columns is None else piece.at[:, columns], place, sem))
    return copies


def _gathered(at_ref, given, rows_s):
    for n, ref in enumerate(given):
        rows_s[pl.ds(pl.multiple_of(at_ref[n], ref.shape[0]), ref.shape[0]), :] = ref[...]
    return rows_s[...]


def _add(acc, here, got):
    @pl.when(pl.program_id(0) == 0)
    def _():
        acc[:, here] = got

    @pl.when(pl.program_id(0) > 0)
    def _():
        acc[:, here] += got


def _qkv_kernel(table_ref, at_ref, *refs, pieces, carried):
    given, (wq_ref, wk_ref, wv_ref, cos_ref, sin_ref, *refs) = refs[:pieces], refs[pieces:]
    q_ref, k_ref, v_ref, rows_s, acc, q_s, k_s, v_s, turns_s, sem, turns_sem = refs[carried:]
    wide = wq_ref.shape[1]
    steps, devices, span, _ = q_s.shape
    places = [(pl.ds(table_ref[i, 0] * devices, devices), table_ref[i, 1]) for i in range(steps)]

    def turns():
        return [pltpu.make_async_copy(ref.at[place], turns_s.at[n, i], turns_sem.at[n, i])
                for n, ref in enumerate((cos_ref, sin_ref)) for i, place in enumerate(places)]

    @pl.when(pl.program_id(0) == 0)
    def _():
        for copy in turns():
            copy.start()

    rows = _gathered(at_ref, given, rows_s)
    _add(acc, slice(0, wide), _dot(rows, wq_ref[...], 1, 0))
    _add(acc, slice(wide, wide + 2 * HEAD), _dot(rows, jnp.concatenate([wk_ref[...], wv_ref[...]], axis=1), 1, 0))

    @pl.when(pl.program_id(0) == pl.num_programs(0) - 1)
    def _():
        for copy in turns():
            copy.wait()
        copies = []
        for i, to in enumerate(places):
            for d in range(devices):
                here = slice((i * devices + d) * span, (i * devices + d + 1) * span)
                cos, sin = turns_s[0, i, d], turns_s[1, i, d]
                for h in range(0, wide, HEAD):
                    q_s[i, d, :, h : h + HEAD] = _turn(acc[here, h : h + HEAD], cos, sin)
                k_s[i, d] = _turn(acc[here, wide : wide + HEAD], cos, sin)
                v_s[i, d] = acc[here, wide + HEAD :].astype(jnp.bfloat16)
            for n, (scratch, ref) in enumerate(((q_s, q_ref), (k_s, k_ref), (v_s, v_ref))):
                copies.append(pltpu.make_async_copy(scratch.at[i], ref.at[to], sem.at[i, n]))
                copies[-1].start()
        for copy in copies:
            copy.wait()


def _step_spec(span, wide):
    return pl.BlockSpec((DEVS, 1, span, wide), lambda i, table, *_: (table[i, 0], table[i, 1], 0, 0))


def qkv(table, at, pieces, weights, cos, sin, sofar, chunks=4):
    devices, parts, span, _ = cos.shape
    depth = weights[0].shape[0]
    widths = [t.shape[1] for t in weights]
    steps, tile = table.shape[0], depth // chunks
    rows = steps * DEVS * span
    sofar = sofar or ()
    any_ = pl.BlockSpec(memory_space=pl.ANY)
    return pl.pallas_call(
        functools.partial(_qkv_kernel, pieces=len(pieces), carried=len(sofar)),
        grid_spec=pltpu.PrefetchScalarGridSpec(
            num_scalar_prefetch=2,
            grid=(chunks,),
            in_specs=[*(pl.BlockSpec((t.shape[0], tile), lambda i, *_: (0, i)) for t in pieces), *(pl.BlockSpec((tile, n), lambda i, *_: (i, 0)) for n in widths),
                      any_, any_, *(any_ for _ in sofar)],
            out_specs=[any_ for _ in widths],
            scratch_shapes=[pltpu.VMEM((rows, tile), jnp.bfloat16), pltpu.VMEM((rows, sum(widths)), jnp.float32),
                            *(pltpu.VMEM((steps, DEVS, span, n), jnp.bfloat16) for n in widths), pltpu.VMEM((2, steps, DEVS, span, HEAD), jnp.float32),
                            pltpu.SemaphoreType.DMA((steps, len(widths))), pltpu.SemaphoreType.DMA((2, steps))],
        ),
        out_shape=[_like((devices, parts, span, n)) for n in widths],
        input_output_aliases={2 + len(pieces) + len(widths) + 2 + n: n for n in range(len(sofar))},
        compiler_params=_params(),
        cost_estimate=pl.CostEstimate(flops=2 * rows * depth * sum(widths), transcendentals=0, bytes_accessed=2 * depth * (rows + sum(widths))),
        name="qkv",
    )(table, at, *pieces, *weights, cos, sin, *sofar)


def _wo_kernel(at_ref, *refs, pieces):
    given, (w_ref, o_ref, rows_s, acc) = refs[:pieces], refs[pieces:]
    _add(acc, slice(None), _dot(_gathered(at_ref, given, rows_s), w_ref[...], 1, 1))

    @pl.when(pl.program_id(0) == pl.num_programs(0) - 1)
    def _():
        o_ref[...] = acc[...].astype(jnp.bfloat16)


def back_through_wo(at, pieces, wo, chunks=4):
    rows, (wide, depth) = sum(p.shape[0] for p in pieces), wo.shape
    tile = depth // chunks
    return pl.pallas_call(
        functools.partial(_wo_kernel, pieces=len(pieces)),
        grid_spec=pltpu.PrefetchScalarGridSpec(
            num_scalar_prefetch=1,
            grid=(chunks,),
            in_specs=[*(pl.BlockSpec((t.shape[0], tile), lambda i, at: (0, i)) for t in pieces), pl.BlockSpec((wide, tile), lambda i, at: (0, i))],
            out_specs=_whole((rows, wide)),
            scratch_shapes=[pltpu.VMEM((rows, tile), jnp.bfloat16), pltpu.VMEM((rows, wide), jnp.float32)],
        ),
        out_shape=_like((rows, wide)),
        compiler_params=_params(),
        cost_estimate=pl.CostEstimate(flops=2 * rows * depth * wide, transcendentals=0, bytes_accessed=2 * depth * (rows + wide)),
        name="back_through_wo",
    )(at, *pieces, wo)


def _gaps(span):
    column = lax.broadcasted_iota(jnp.int32, (BK, DEVS * span), 1)
    place = (column // span) * (span * PARTS) + column % span
    return place - lax.broadcasted_iota(jnp.int32, (BK, DEVS * span), 0)


def _part(ref, h):
    return ref[:, 0, :, h * HEAD : (h + 1) * HEAD].reshape(-1, HEAD)


def _forward(q_ref, k_ref, v_ref, o_ref, lse_ref, top_s, mix_s, gap_s):
    chip, half = pl.program_id(0), pl.program_id(1)
    span = q_ref.shape[2]
    heads = q_ref.shape[-1] // HEAD
    scale = HEAD**-0.5
    e = scale * LOG2E

    @pl.when((chip == 0) & (half == 0))
    def _():
        gap_s[...] = _gaps(span)

    top_s[...] = jnp.full(top_s.shape, NEG, jnp.float32)
    mix_s[...] = jnp.zeros(mix_s.shape, jnp.float32)

    def step(j, masked):
        here = pl.ds(pl.multiple_of(j * BK, BK), BK)
        k = k_ref[here, :]
        values = jnp.concatenate([v_ref[here, :].T, jnp.ones((8, BK), jnp.bfloat16)], axis=0)
        scores = [_dot(k, _part(q_ref, h), 1, 1) for h in range(heads)]
        weights, keeps = [], []
        for h, s in enumerate(scores):
            if masked:
                s = jnp.where(gap_s[...] >= -half * span, s, HIDDEN)
            old = top_s[h : h + 1, :]
            top = jnp.maximum(old, s.max(axis=0, keepdims=True))
            top_s[h : h + 1, :] = top
            weights.append(jnp.exp2((s - top) * e).astype(jnp.bfloat16))
            keeps.append(jnp.exp2((old - top) * e))
        for h in range(heads):
            mix_s[h] = mix_s[h] * keeps[h] + _dot(values, weights[h], 1, 0)

    lax.fori_loop(0, chip, lambda j, _: step(j, False), None)
    step(chip, True)
    for h in range(heads):
        total = mix_s[h, HEAD : HEAD + 1, :]
        o_ref[:, 0, :, h * HEAD : (h + 1) * HEAD] = (mix_s[h, :HEAD, :] * (1 / total)).T.astype(jnp.bfloat16).reshape(DEVS, span, HEAD)
        lse_ref[0, 0, h : h + 1, :] = top_s[h : h + 1, :] * scale + jnp.log(total)


def attend(q, k, v):
    devices, parts, span, wide = q.shape
    heads, nq, keys = wide // HEAD, DEVS * span, k.shape[0]
    chips = devices // DEVS
    part = pl.BlockSpec((DEVS, 1, span, wide), lambda i, j: (i, j, 0, 0))
    return pl.pallas_call(
        _forward,
        grid=(chips, parts),
        in_specs=[part, _whole(k.shape), _whole(v.shape)],
        out_specs=[part, pl.BlockSpec((1, 1, heads, nq), lambda i, j: (i, j, 0, 0))],
        out_shape=[_like(q.shape), _like((chips, parts, heads, nq), jnp.float32)],
        scratch_shapes=[pltpu.VMEM((heads, nq), jnp.float32), pltpu.VMEM((heads, HEAD + 8, nq), jnp.float32), pltpu.VMEM((BK, nq), jnp.int32)],
        compiler_params=_params(2),
        cost_estimate=_cost(2 * q.size * keys * 2, [q, k, v, q], q.size // HEAD * keys),
        name="attend",
    )(q, k, v)


def _backward(table_ref, *refs, first, last):
    q_ref, k_ref, v_ref, do_ref, o_ref, lse_ref, cos_ref, sin_ref, *refs = refs
    if not first:
        dk_in, dv_in, _, *refs = refs
    if last:
        kcos_ref, ksin_ref, dq_ref, dkv_ref, *refs = refs
    else:
        dq_ref, dk_ref, dv_ref, *refs = refs
    dq_s, dk_s, dv_s, gap_s = refs
    i = pl.program_id(0)
    chip, half = table_ref[i, 0], table_ref[i, 1]
    span = q_ref.shape[2]
    heads = q_ref.shape[-1] // HEAD
    scale = HEAD**-0.5
    e = scale * LOG2E

    @pl.when(i == 0)
    def _():
        gap_s[...] = _gaps(span)
        dk_s[...] = jnp.zeros(dk_s.shape, jnp.float32) if first else dk_in[...]
        dv_s[...] = jnp.zeros(dv_s.shape, jnp.float32) if first else dv_in[...]

    dq_s[...] = jnp.zeros(dq_s.shape, jnp.float32)
    head = lambda ref, h: ref[:, h * HEAD : (h + 1) * HEAD]
    lses = [lse_ref[0, 0, h : h + 1, :] * LOG2E for h in range(heads)]
    deltas = [(head(do_ref, h).astype(jnp.float32) * _part(o_ref, h).astype(jnp.float32)).T.sum(axis=0, keepdims=True) for h in range(heads)]

    def step(j, masked):
        here = pl.ds(pl.multiple_of(j * BK, BK), BK)
        k, v = k_ref[here, :], v_ref[here, :]
        kt = k.T
        scores = [_dot(k, _part(q_ref, h), 1, 1) for h in range(heads)]
        dps = [_dot(v, head(do_ref, h), 1, 1) for h in range(heads)]
        for h in range(heads):
            w = jnp.exp2(scores[h] * e - lses[h])
            if masked:
                w = jnp.where(gap_s[...] >= -half * span, w, 0.0)
            ds = (w * (dps[h] - deltas[h])).astype(jnp.bfloat16)
            dv_s[here, :] += _dot(w.astype(jnp.bfloat16), head(do_ref, h), 1, 0)
            dk_s[here, :] += _dot(ds, _part(q_ref, h), 1, 0)
            dq_s[h] += _dot(kt, ds, 1, 0)

    lax.fori_loop(0, chip, lambda j, _: step(j, False), None)
    step(chip, True)
    cos, sin = (r[:, 0].reshape(-1, HEAD) for r in (cos_ref, sin_ref))
    for h in range(heads):
        dq_ref[:, 0, 0, :, h * HEAD : (h + 1) * HEAD] = _turn((dq_s[h] * scale).T, cos, -sin).reshape(DEVS, span, HEAD)

    @pl.when(i == pl.num_programs(0) - 1)
    def _():
        if last:
            dkv_ref[:, :HEAD] = _turn(dk_s[...] * scale, kcos_ref[...], -ksin_ref[...])
            dkv_ref[:, HEAD:] = dv_s[...].astype(jnp.bfloat16)
        else:
            dk_ref[...] = dk_s[...]
            dv_ref[...] = dv_s[...]


def attend_bwd(table, q, k, v, d_out, skip, out, lse, cos, sin, sofar, last):
    devices, parts, span, wide = q.shape
    heads, nq, keys = wide // HEAD, DEVS * span, k.shape[0]
    chips = devices // DEVS
    steps = table.shape[0]
    kv = _whole(k.shape)
    dq_shape = (DEVS, chips, parts, span, wide)
    more, specs = [], []
    if sofar is not None:
        dq, dk, dv = sofar
        more, specs = [dk, dv, dq], [kv, kv, pl.BlockSpec(memory_space=pl.ANY)]
    if last:
        more, specs = [*more, cos.reshape(keys, HEAD), sin.reshape(keys, HEAD)], [*specs, kv, kv]
    sums = [(keys, 2 * HEAD)] if last else [k.shape, k.shape]
    return pl.pallas_call(
        functools.partial(_backward, first=sofar is None, last=last),
        grid_spec=pltpu.PrefetchScalarGridSpec(
            num_scalar_prefetch=1,
            grid=(steps,),
            in_specs=[_step_spec(span, wide), kv, kv, pl.BlockSpec((nq, wide), lambda i, table: (i + skip, 0)), _step_spec(span, wide),
                      pl.BlockSpec((1, 1, heads, nq), lambda i, table: (table[i, 0], table[i, 1], 0, 0)),
                      _step_spec(span, HEAD), _step_spec(span, HEAD), *specs],
            out_specs=[pl.BlockSpec((DEVS, 1, 1, span, wide), lambda i, table: (0, table[i, 0], table[i, 1], 0, 0)), *(_whole(t) for t in sums)],
            scratch_shapes=[pltpu.VMEM((heads, HEAD, nq), jnp.float32), pltpu.VMEM((keys, HEAD), jnp.float32),
                            pltpu.VMEM((keys, HEAD), jnp.float32), pltpu.VMEM((BK, nq), jnp.int32)],
        ),
        out_shape=[_like(dq_shape), *(_like(t, jnp.bfloat16 if last else jnp.float32) for t in sums)],
        input_output_aliases={} if sofar is None else {11: 0},
        compiler_params=_params(),
        cost_estimate=pl.CostEstimate(flops=2 * steps * nq * wide * keys * 5, transcendentals=steps * nq * heads * keys, bytes_accessed=8 * steps * nq * wide),
        name="attend_bwd",
    )(table, q, k, v, d_out, out, lse, cos, sin, *more)


def _da_kernel(core_ref, dq_ref, dkv_ref, pq_ref, pkv_ref, wq_ref, wk_ref, wv_ref, pwq_ref, pwk_ref, pwv_ref, o_ref, kv_s):
    chips, parts, span, wide = pq_ref.shape
    rows = chips * parts * span

    @pl.when(pl.program_id(0) == 0)
    def _():
        kv_s[:, : 2 * HEAD] = dkv_ref[:, 0].reshape(rows, 2 * HEAD)
        kv_s[:, 2 * HEAD :] = pkv_ref[...].reshape(rows, 2 * HEAD)

    wkv = jnp.concatenate([r[...] for r in (wk_ref, wv_ref, pwk_ref, pwv_ref)], axis=1)
    got = _dot(dq_ref[0].reshape(rows, wide), wq_ref[...], 1, 1) + _dot(pq_ref[...].reshape(rows, wide), pwq_ref[...], 1, 1)
    o_ref[...] = (got + _dot(kv_s[...], wkv, 1, 1)).astype(jnp.bfloat16)


def grad_a(core, dq, dkv, pq, pkv, weights, others, first, columns, tile=512):
    chips, parts, span, wide = pq.shape
    block = parts * span
    rows = chips * block
    skip = first // tile
    once = dict(pipeline_mode=pl.Buffered(1))
    return pl.pallas_call(
        _da_kernel,
        grid_spec=pltpu.PrefetchScalarGridSpec(
            num_scalar_prefetch=1,
            grid=(columns // tile,),
            in_specs=[pl.BlockSpec((1, chips, parts, span, wide), lambda i, core: (core[0], 0, 0, 0, 0), **once),
                      pl.BlockSpec((chips, 1, block, 2 * HEAD), lambda i, core: (0, core[0], 0, 0), **once),
                      _whole(pq.shape), _whole(pkv.shape), *(pl.BlockSpec((tile, t.shape[1]), lambda i, core: (i + skip, 0)) for t in (*weights, *others))],
            out_specs=pl.BlockSpec((rows, tile), lambda i, core: (0, i)),
            scratch_shapes=[pltpu.VMEM((rows, 4 * HEAD), jnp.bfloat16)],
        ),
        out_shape=_like((rows, columns)),
        compiler_params=_params(),
        cost_estimate=pl.CostEstimate(flops=4 * rows * columns * (wide + 2 * HEAD), transcendentals=0, bytes_accessed=4 * columns * (wide + 2 * HEAD)),
        name="grad_a",
    )(core, dq, dkv, pq, pkv, *weights, *others)


def _columns_here(at_ref, pieces, rows_s, sem):
    i, steps = pl.program_id(0), pl.num_programs(0)
    tile = rows_s.shape[-1]

    def copies(step):
        slot = lax.rem(step, 2)
        return _fetch(at_ref, pieces, rows_s.at[slot], sem.at[slot], pl.ds(pl.multiple_of(step * tile, tile), tile))

    @pl.when(i == 0)
    def _():
        for copy in copies(i):
            copy.start()

    @pl.when(i + 1 < steps)
    def _():
        for copy in copies(i + 1):
            copy.start()

    for copy in copies(i):
        copy.wait()
    return rows_s[lax.rem(i, 2)]


def _dw_kernel(at_ref, *refs, pieces):
    given, (dq_ref, dkv_ref, oq_ref, ok_ref, ov_ref, cat_s, rows_s, sem) = refs[:pieces], refs[pieces:]
    wide = oq_ref.shape[1]

    @pl.when(pl.program_id(0) == 0)
    def _():
        cat_s[:, wide:] = dkv_ref[...]
        cores, chips, parts, span, _ = dq_ref.shape
        for chip in range(chips):
            for core in range(cores):
                for n in range(parts):
                    at = ((chip * cores + core) * parts + n) * span
                    cat_s[at : at + span, :wide] = dq_ref[core, chip, n]

    got = _dot(_columns_here(at_ref, given, rows_s, sem), cat_s[...], 0, 0)
    oq_ref[...] = got[:, :wide].astype(jnp.bfloat16)
    ok_ref[...] = got[:, wide : wide + HEAD].astype(jnp.bfloat16)
    ov_ref[...] = got[:, wide + HEAD :].astype(jnp.bfloat16)


def grad_qkv(at, pieces, dq, dkv, tile=512):
    rows, depth, wide = dkv.shape[0], pieces[0].shape[1], dq.shape[-1]
    shapes = [(depth, wide), (depth, HEAD), (depth, HEAD)]
    return pl.pallas_call(
        functools.partial(_dw_kernel, pieces=len(pieces)),
        grid_spec=pltpu.PrefetchScalarGridSpec(
            num_scalar_prefetch=1,
            grid=(depth // tile,),
            in_specs=[*(pl.BlockSpec(memory_space=pl.ANY) for _ in pieces), _whole(dq.shape), _whole(dkv.shape)],
            out_specs=[pl.BlockSpec((tile, t[1]), lambda i, at: (i, 0)) for t in shapes],
            scratch_shapes=[pltpu.VMEM((rows, wide + 2 * HEAD), jnp.bfloat16), pltpu.VMEM((2, rows, tile), jnp.bfloat16), pltpu.SemaphoreType.DMA((2,))],
        ),
        out_shape=[_like(t) for t in shapes],
        compiler_params=_params(),
        cost_estimate=_cost(2 * rows * depth * (wide + 2 * HEAD), [*pieces, dq, dkv]),
        name="grad_qkv",
    )(at, *pieces, dq, dkv)


def _dwo_kernel(at_ref, *refs, pieces):
    given, (out_ref, o_ref, rows_s, sem) = refs[:pieces], refs[pieces:]
    o_ref[...] = _dot(out_ref[...], _columns_here(at_ref, given, rows_s, sem), 0, 0).astype(jnp.bfloat16)


def grad_wo(at, pieces, out, tile=512):
    depth, (rows, wide) = pieces[0].shape[1], out.shape
    return pl.pallas_call(
        functools.partial(_dwo_kernel, pieces=len(pieces)),
        grid_spec=pltpu.PrefetchScalarGridSpec(
            num_scalar_prefetch=1,
            grid=(depth // tile,),
            in_specs=[*(pl.BlockSpec(memory_space=pl.ANY) for _ in pieces), _whole(out.shape)],
            out_specs=pl.BlockSpec((wide, tile), lambda i, at: (0, i)),
            scratch_shapes=[pltpu.VMEM((2, rows, tile), jnp.bfloat16), pltpu.SemaphoreType.DMA((2,))],
        ),
        out_shape=_like((wide, depth)),
        compiler_params=_params(),
        cost_estimate=_cost(2 * rows * depth * wide, [*pieces, out]),
        name="grad_wo",
    )(at, *pieces, out)


def _norm_kernel(*refs):
    x_ref, dy_ref, gain_ref, *das, o_ref, og_ref = refs
    x = x_ref[...].astype(jnp.float32)
    scale = lax.rsqrt(jnp.mean(x * x, -1, keepdims=True) + 1e-6)
    da = jnp.concatenate([r[...].astype(jnp.float32) for r in das], axis=1)
    unit = x * scale
    by_unit = da * gain_ref[...].astype(jnp.float32)
    mean = jnp.mean(by_unit * unit, -1, keepdims=True)
    o_ref[...] = (dy_ref[...].astype(jnp.float32) + scale * (by_unit - unit * mean)).astype(jnp.bfloat16)
    part = jnp.sum(da * unit, axis=0, keepdims=True)

    @pl.when(pl.program_id(0) == 0)
    def _():
        og_ref[...] = part

    @pl.when(pl.program_id(0) > 0)
    def _():
        og_ref[...] += part


def norm_bwd(x, dy, gain, das, tile=64):
    rows, depth = x.shape
    row = lambda n: pl.BlockSpec((tile, n), lambda i: (i, 0))
    return pl.pallas_call(
        _norm_kernel,
        grid=(rows // tile,),
        in_specs=[row(depth), row(depth), _whole((1, depth)), *(row(d.shape[1]) for d in das)],
        out_specs=[row(depth), pl.BlockSpec((1, depth), lambda i: (0, 0))],
        out_shape=[_like((rows, depth)), _like((1, depth), jnp.float32)],
        compiler_params=_params(),
        cost_estimate=_cost(20 * rows * depth, [x, dy, x, x]),
        name="norm_bwd",
    )(x, dy, gain.reshape(1, depth), *das)


def _share_kernel(n, mine_ref, o_ref, held, send_sem, recv_sem):
    me = lax.axis_index("tp")
    barrier = pltpu.get_barrier_semaphore()
    for d in range(1, n):
        pl.semaphore_signal(barrier, inc=1, device_id={"tp": lax.rem(me + d, n)}, device_id_type=pl.DeviceIdType.MESH)
    pl.semaphore_wait(barrier, n - 1)
    copies = []
    for d in range(1, n):
        copy = pltpu.make_async_remote_copy(src_ref=mine_ref, dst_ref=held.at[d - 1], send_sem=send_sem.at[d - 1], recv_sem=recv_sem.at[d - 1],
                                            device_id={"tp": lax.rem(me + d, n)}, device_id_type=pl.DeviceIdType.MESH)
        copy.start()
        copies.append(copy)
    for copy in copies:
        copy.wait()
    total = jnp.zeros(o_ref.shape, jnp.float32)
    for i in range(n):
        other = held[jnp.maximum(lax.rem(me - i + n, n) - 1, 0)]
        total += jnp.where(me == i, mine_ref[...], other)
    o_ref[...] = total


def share_sum(part, n):
    return pl.pallas_call(
        functools.partial(_share_kernel, n),
        in_specs=[pl.BlockSpec(memory_space=pltpu.VMEM)],
        out_specs=pl.BlockSpec(memory_space=pltpu.VMEM),
        out_shape=_like(part.shape, jnp.float32),
        scratch_shapes=[pltpu.VMEM((n - 1, *part.shape), jnp.float32), pltpu.SemaphoreType.DMA((n - 1,)), pltpu.SemaphoreType.DMA((n - 1,))],
        compiler_params=pltpu.CompilerParams(collective_id=0, has_side_effects=True),
        cost_estimate=pl.CostEstimate(flops=n * part.size, transcendentals=0, bytes_accessed=8 * part.size),
        name="share_sum",
    )(part)


def solution(mesh):
    n = mesh.shape["tp"]
    chips = n // DEVS
    same = [list(range(c, n, DEVS)) for c in range(DEVS)]
    other = [(i, i ^ 1) for i in range(n)]
    right = [(i, (i + DEVS) % n) for i in range(n)]
    left = [(i, (i - DEVS) % n) for i in range(n)]

    def program(x, dy, gain, wq, wk, wv, wo):
        block, depth = x.shape
        rows = n * block
        span = block // PARTS
        me = lax.axis_index("tp")
        core, chip = lax.rem(me, DEVS), lax.div(me, DEVS)

        def send(t, ring):
            return lax.ppermute(t, "tp", ring)

        places = lambda *steps: jnp.stack([jnp.stack([lax.rem(chip + shift, chips), jnp.full_like(chip, half)]) for shift, half in steps])
        tables = [places((0, 0), (0, 1)), places((chips - 1, 0), (1, 1)), places((chips - 1, 1), (1, 0)), places((2, 0), (2, 1))]

        def gather(t):
            top, low = t
            from_left0, from_right1 = send(top, right), send(low, left)
            from_left1, from_right0 = send(low, right), send(top, left)
            across0, across1 = send(from_left0, right), send(from_right1, left)
            groups = [(top, low), (from_left0, from_right1), (from_left1, from_right0), (across0, across1)]
            return [(*g, *(send(p, other) for p in g)) for g in groups]

        near = jnp.stack([core * span, block + core * span, (1 - core) * span, block + (1 - core) * span])
        far = jnp.concatenate([jnp.concatenate([(t[:, 0] * DEVS + c) * block + t[:, 1] * span for c in (core, 1 - core)]) for t in tables])

        half = HEAD // 2
        angle = jnp.arange(rows, dtype=jnp.float32)[:, None] * THETA ** (-jnp.arange(half, dtype=jnp.float32) / half)
        cos, sin = jnp.cos(angle), jnp.sin(angle)
        cos, sin = lax.optimization_barrier((jnp.concatenate([cos, cos], 1), jnp.concatenate([-sin, sin], 1)))
        cos, sin = (t.reshape(n, PARTS, span, HEAD) for t in (cos, sin))

        top, low = normed(x, gain)
        xs = gather((top, low))
        later, _ = lax.optimization_barrier((dy, low))
        later = later[:span], later[span:]
        dys = gather(later)
        weights = wq, wk, wv
        others = [send(t, other) for t in weights]
        got = None
        for table, pieces in zip(tables, xs):
            got = qkv(table, near, pieces, weights, cos, sin, got)
        q, k, v = got
        k, v = k.reshape(rows, HEAD), v.reshape(rows, HEAD)
        out, lse = attend(q, k, v)
        got = None
        for i, table in enumerate(tables):
            if i != 2:
                at, pieces = (jnp.concatenate([near, near + DEVS * block]), [*dys[1], *dys[2]]) if i == 1 else (near, dys[i])
                d_out = back_through_wo(at, pieces, wo)
            got = attend_bwd(table, q, k, v, d_out, 2 if i == 2 else 0, out, lse, cos, sin, got, i == len(tables) - 1)
        dq, dkv = got
        dkvs = dkv.reshape(chips, DEVS, block, 2 * HEAD)
        pq = send(lax.dynamic_index_in_dim(dq, 1 - core, 0, False), other)
        pkv = send(lax.dynamic_index_in_dim(dkvs, 1 - core, 1, False), other)
        das, first = [], 0
        for share in COLS:
            width = depth * share // sum(COLS)
            term = grad_a(core[None], dq, dkvs, pq, pkv, weights, others, first, width)
            first += width
            das.append(lax.psum_scatter(term, "tp", scatter_dimension=0, axis_index_groups=same, tiled=True))
        flat = lambda groups: [p for g in groups for p in g]
        by_wo = grad_wo(far, flat(dys), out.reshape(rows, -1))
        by_qkv = grad_qkv(far, flat(xs), dq, dkv)
        by_x, by_gain = norm_bwd(x, dy, gain, das)
        return by_x, share_sum(by_gain, n), *by_qkv, by_wo

    tokens, columns = P(("dp", "tp"), None), P(None, "tp")
    return jax.shard_map(
        program,
        mesh=mesh,
        in_specs=(tokens, tokens, P(None), columns, columns, columns, P("tp", None)),
        out_specs=(tokens, P("dp", None), P("dp", "tp"), P("dp", "tp"), P("dp", "tp"), P(("dp", "tp"), None)),
        check_vma=False,
    )
```
